32 devices in a mesh: node: 8 (over z, y), local: 4 (over x, core).
Axes of the slice: x: 2, y: 2, z: 4, core: 2. Of those that a mesh axis runs over, the one named last changes fastest.
Arguments:
- tokens: bfloat16 [4096, 2048], P(('node', 'local')), may hold values from -6 to 6
- norm_gain: float32 [2048], replicated, may hold values from 0.1 to 1.9
- router_weight: bfloat16 [2048, 16], replicated, may hold values from -0.125 to 0.125
- placement: int32 [16], replicated, may hold values from 0 to 15, each once
- expert_ids: int32 [4096, 6], P(('node', 'local')), may hold values from 0 to 15, all different within a row; in each aligned block of 128 rows (0 to 127, 128 to 255, ...) at most 72 rows name the same one
- w_gate: bfloat16 [2048, 22528], P(None, ('node', 'local')), may hold values from -0.125 to 0.125
- w_up: bfloat16 [2048, 22528], P(None, ('node', 'local')), may hold values from -0.125 to 0.125
- w_down: bfloat16 [22528, 2048], P(('node', 'local')), may hold values from -0.15625 to 0.15625
- shared_gate: bfloat16 [2048, 2816], P(None, 'local'), may hold values from -0.125 to 0.125
- shared_up: bfloat16 [2048, 2816], P(None, 'local'), may hold values from -0.125 to 0.125
- shared_down: bfloat16 [2816, 2048], P('local'), may hold values from -0.109375 to 0.109375
Outputs:
- moe_out: bfloat16 [4096, 2048], P(('node', 'local'))
The draws below stay inside these ranges and needn't reach their ends.
Inputs may be any that keep to these rules, and one draw needn't show every extreme that they name: Expert e's weights stand in slot placement[e]; every slot holds one expert. `expert_ids`: each row names 6 different experts. Among the rows of one device (aligned blocks of 128 rows) no expert is named more than 72 times, a bound that some block reaches.
All inputs are finite; a program needn't handle non-finite values.
Results may differ from the reference program's by a relative error of at most 0.011.
Values may be sent and summed in bfloat16 or wider, within the bound.
No kernel may reach another device: no remote copies, remote signals or barrier semaphores. Data moves between devices by JAX's collectives and lax.ppermute only.
A program may use at most 128 MiB of HBM per device.

```python
import math
import jax
import jax.numpy as jnp
import numpy as np
from jax import lax

D = 2048
FE = 1408
FS = 2816
TOPK = 6
TOK_DEV = 128
EXPERTS = 16
HALF = 704
CAP = 72
TOKENS = 4096
DEVICES = 32


def levels(key, dims, shards, smallest, high):
    def one(dim, shards_of):
        draws = jax.random.uniform(jax.random.fold_in(jax.random.fold_in(key, 6), dim), (shards_of,), jnp.float32, smallest / len(shards), high / len(shards))
        return jnp.repeat(jnp.exp(draws), dims[dim] // shards_of).reshape((-1,) + (1,) * (len(dims) - dim - 1))

    gain = one(*shards[0])
    for cut in shards[1:]:
        gain = gain * one(*cut)
    return gain


def routed_block(rng, own, number, rows, number_of, top, most, slope):
    order = jax.random.permutation(rng, number_of)
    packed, usual = portions_of(number_of, rows * top, most, slope, True), portions_of(number_of, rows * top, most, slope, False)
    places = jnp.arange(number_of)

    def named(tallies, turn):
        used = int((tallies > 0).sum())
        fixed = max(1, used // 4)
        moved = fixed + (places - fixed + turn * (used - fixed)) % max(1, number_of - fixed)
        return jnp.zeros((number_of,), jnp.int32).at[order[jnp.where(places < fixed, places, moved)]].set(jnp.asarray(tallies, jnp.int32))

    tallies = jnp.where(number % 4 == 0, named(packed, number // 4), named(usual, number - number // 4 - 1))
    mixed = jax.random.permutation(jax.random.fold_in(own, 3), number_of)
    giver, receiver = mixed[0:number_of // 2 * 2:2], mixed[1:number_of // 2 * 2:2]
    room = jnp.minimum(tallies[giver] - 1, most - tallies[receiver]) // 2
    room = jnp.where((giver == order[0]) | (receiver == order[0]) | (tallies[receiver] == 0), 0, jnp.maximum(room, 0))
    moved = jax.random.randint(jax.random.fold_in(own, 4), (number_of // 2,), 0, 1 << 20) % (room + 1)
    tallies = tallies.at[giver].add(-moved).at[receiver].add(moved)
    items = jnp.searchsorted(jnp.cumsum(tallies), jnp.arange(rows * top), side="right").astype(jnp.int32)
    grid = items.reshape(top, rows).T
    grid = grid[jax.random.permutation(jax.random.fold_in(own, 1), rows)]
    turn = jax.random.randint(jax.random.fold_in(own, 2), (rows, 1), 0, top)
    return jnp.take_along_axis(grid, (jnp.arange(top)[None, :] + turn) % top, axis=1)


def portions_of(number_of, total, reach, lean, full):
    portions = [(1 << 20) // math.isqrt(rank ** lean) + 1 for rank in range(1, number_of + 1)]
    largest = reach if full else min(reach, max(-(-total // number_of), total * portions[0] // sum(portions)))
    least = 1 if total - largest >= number_of - 1 else 0
    counts, surplus = [largest] + [least] * (number_of - 1), total - largest - least * (number_of - 1)
    while surplus > 0:
        candidates = [i for i in range(1, number_of) if counts[i] < largest] or [i for i in range(1, number_of) if counts[i] < reach]
        whole, left = sum([portions[i] for i in candidates]), surplus
        for i in candidates:
            addition = min(reach - counts[i], max(1, left * portions[i] // whole), surplus)
            counts[i] = counts[i] + addition
            surplus = surplus - addition
    return np.array(counts)


def centred(stream_key, shape, width, most, cuts=(), held_as=jnp.bfloat16):
    factor_of = levels(stream_key, shape, cuts, -0.22, 0.18) if cuts else 1.0
    array = jax.random.normal(stream_key, shape, jnp.float32) * width * factor_of
    return jnp.minimum(jnp.maximum(array, -most), most).astype(held_as)


def setup_inputs(seed: int = 0) -> dict:
    streams_of = jax.random.split(jax.random.key(seed), 12)
    tokens = centred(streams_of[0], (TOKENS, D), 1.0, 6.0, ((0, 32),))
    norm_gain = jnp.clip(1.0 + 0.18 * jax.random.normal(streams_of[1], (D,), jnp.float32), 0.1, 1.9)
    router_weight = centred(streams_of[2], (D, EXPERTS), D ** -0.5, 0.125)
    placement = jax.random.permutation(streams_of[3], EXPERTS).astype(jnp.int32)
    expert_ids_keys = jax.random.split(jax.random.fold_in(streams_of[4], 1), TOKENS // TOK_DEV)
    expert_ids_turns = jax.random.permutation(jax.random.fold_in(streams_of[4], 3), TOKENS // TOK_DEV)
    expert_ids = jax.vmap(lambda own, number: routed_block(jax.random.fold_in(streams_of[4], 2), own, number, TOK_DEV, EXPERTS, TOPK, CAP, 2))(expert_ids_keys, expert_ids_turns).reshape((TOKENS, TOPK))
    w_gate = centred(streams_of[5], (D, EXPERTS * FE), D ** -0.5, 0.125, ((1, 32),))
    w_up = centred(streams_of[6], (D, EXPERTS * FE), D ** -0.5, 0.125, ((1, 32),))
    w_down = centred(streams_of[7], (EXPERTS * FE, D), FE ** -0.5, 0.15625, ((0, 32),))
    shared_gate = centred(streams_of[8], (D, FS), D ** -0.5, 0.125, ((1, 4),))
    shared_up = centred(streams_of[9], (D, FS), D ** -0.5, 0.125, ((1, 4),))
    shared_down = centred(streams_of[10], (FS, D), FS ** -0.5, 0.109375, ((0, 4),))
    return dict(tokens=tokens, norm_gain=norm_gain, router_weight=router_weight, placement=placement, expert_ids=expert_ids, w_gate=w_gate, w_up=w_up, w_down=w_down, shared_gate=shared_gate, shared_up=shared_up, shared_down=shared_down)


def feed_forward(row_block, gate_cols, up_cols, down_rows):
    gate_proj = jnp.dot(row_block, gate_cols, preferred_element_type=jnp.float32)
    up_proj = jnp.dot(row_block, up_cols, preferred_element_type=jnp.float32)
    activated = (jax.nn.silu(gate_proj) * up_proj).astype(jnp.bfloat16)
    return jnp.dot(activated, down_rows, preferred_element_type=jnp.float32)

def reference(tokens, norm_gain, router_weight, placement, expert_ids, w_gate, w_up, w_down, shared_gate, shared_up, shared_down):
    floats = tokens.astype(jnp.float32)
    normed = (floats * lax.rsqrt(lax.optimization_barrier(jnp.mean(floats * floats, -1, keepdims=True)) + 1e-06) * norm_gain).astype(jnp.bfloat16)
    logits = jnp.dot(normed, router_weight, preferred_element_type=jnp.float32)
    scores = jax.nn.sigmoid(logits)
    picked = jnp.take_along_axis(scores, expert_ids, 1)
    gate_weights = (picked / lax.optimization_barrier(jnp.sum(picked, -1, keepdims=True))).astype(jnp.bfloat16)
    slots = placement[expert_ids].astype(jnp.int32)
    expert_iota = jnp.arange(EXPERTS, dtype=jnp.int32)
    slot_hot = (slots[:, :, None] == expert_iota).astype(jnp.int32).reshape(DEVICES, TOK_DEV * TOPK, EXPERTS)
    position = lax.optimization_barrier(jnp.sum((jnp.cumsum(slot_hot, 1) - 1) * slot_hot, -1)).astype(jnp.int32)
    source = jnp.broadcast_to(jnp.arange(DEVICES, dtype=jnp.int32)[:, None], (DEVICES, TOK_DEV * TOPK))
    flat_slot = slots.reshape(DEVICES, TOK_DEV * TOPK)
    index = ((flat_slot * DEVICES + source) * CAP + position).reshape(-1).astype(jnp.int32)
    token_index = jnp.repeat(jnp.arange(TOKENS, dtype=jnp.int32), TOPK)
    table = jnp.full((EXPERTS * DEVICES * CAP,), TOKENS, jnp.int32).at[index].set(token_index)
    weight_table = jnp.zeros((EXPERTS * DEVICES * CAP,), jnp.float32).at[index].set(gate_weights.reshape(-1).astype(jnp.float32))
    padded = jnp.concatenate([normed, jnp.zeros((1, D), jnp.bfloat16)], 0)

    def one_slot(running_sum, slot_index):
        begin = (slot_index * DEVICES * CAP).astype(jnp.int32)
        rows_index = lax.dynamic_slice_in_dim(table, begin, DEVICES * CAP)
        row_weights = lax.dynamic_slice_in_dim(weight_table, begin, DEVICES * CAP)
        row_block = padded[rows_index]
        gate_cols = lax.dynamic_slice_in_dim(w_gate, (slot_index * FE).astype(jnp.int32), FE, 1)
        up_cols = lax.dynamic_slice_in_dim(w_up, (slot_index * FE).astype(jnp.int32), FE, 1)
        down_rows = lax.dynamic_slice_in_dim(w_down, (slot_index * FE).astype(jnp.int32), FE, 0)
        total = jnp.zeros((DEVICES * CAP, D), jnp.float32)
        for half_index in range(2):
            lower = half_index * HALF
            partial_value = feed_forward(row_block, gate_cols[:, lower:lower + HALF], up_cols[:, lower:lower + HALF], down_rows[lower:lower + HALF]).astype(jnp.bfloat16)
            total = total + partial_value.astype(jnp.float32)
        expert_out = total.astype(jnp.bfloat16)
        running_sum = running_sum.at[rows_index].add(row_weights[:, None] * expert_out.astype(jnp.float32), mode='drop')
        return (running_sum, None)
    routed, _ = lax.scan(one_slot, jnp.zeros((TOKENS, D), jnp.float32), jnp.arange(EXPERTS, dtype=jnp.int32))
    shared = feed_forward(normed, shared_gate, shared_up, shared_down)
    return (shared + routed).astype(jnp.bfloat16)
```

```python
import math

import jax
import jax.numpy as jnp
from jax import lax
from jax.sharding import PartitionSpec as P

AXES = ("node", "local")
ORDERS = ("xy", "xy", "xy", "xy")
F32 = jnp.float32
BF16 = jnp.bfloat16


def shift(block, dims, axis, step):
    size = math.prod(dims.values())
    stride, extent = 1, 1
    for name in reversed(dims):
        extent = dims[name]
        if name == axis:
            break
        stride *= extent
    route = []
    for source in range(size):
        place = source // stride % extent
        route.append((source, source + ((place + step) % extent - place) * stride))
    return lax.ppermute(block, AXES, route)


def hidden_units(rows, gate_cols, up_cols):
    gate_proj = jnp.dot(rows, gate_cols, preferred_element_type=F32)
    up_proj = jnp.dot(rows, up_cols, preferred_element_type=F32)
    return (jax.nn.silu(gate_proj) * up_proj).astype(BF16)


def feed_forward(rows, slices):
    total = None
    for gate_cols, up_cols, down_rows in slices:
        part = jnp.dot(hidden_units(rows, gate_cols, up_cols), down_rows, preferred_element_type=F32)
        total = part if total is None else total + part
    return total


def routing_rows(normed, router_weight, placement, expert_ids):
    slots = placement.shape[0]
    tok_rows = normed.shape[0]
    slot_iota = jnp.arange(slots, dtype=jnp.int32)
    to_slot = (placement[:, None] == slot_iota).astype(BF16)
    slot_router = jnp.dot(router_weight, to_slot, preferred_element_type=F32).astype(BF16)
    logits = lax.dot_general(slot_router, normed, (((0,), (1,)), ((), ())), preferred_element_type=F32)
    named = expert_ids[:, :, None] == slot_iota
    token_slots = jnp.sum(jnp.where(named, placement, 0), -1)
    hot = jnp.any(token_slots.T[:, None, :] == slot_iota[:, None], 0)
    picked = jnp.where(hot, jax.nn.sigmoid(logits), 0.0)
    gates = picked / jnp.sum(picked, 0, keepdims=True)
    upper = jnp.arange(tok_rows)[:, None] <= jnp.arange(tok_rows)
    running = jnp.dot(hot.astype(BF16), upper.astype(BF16), preferred_element_type=F32)
    return jnp.concatenate([gates, jnp.where(hot, running, 0.0)], 0).astype(BF16)


def pack(rows, width):
    count, lanes = rows.shape
    strips = -(-count // 8)
    rows = jnp.pad(rows, ((0, strips * 8 - count), (0, 0)))
    side = max(1, width // lanes)
    levels = -(-strips // side)
    rows = jnp.pad(rows, ((0, (levels * side - strips) * 8), (0, 0)))
    packed = rows.reshape(levels, side, 8, lanes).transpose(0, 2, 1, 3).reshape(levels * 8, side * lanes)
    return jnp.pad(packed, ((0, 0), (0, width - side * lanes)))


def unpack(packed, count, lanes):
    levels, width = packed.shape[0] // 8, packed.shape[1]
    side = max(1, width // lanes)
    rows = packed[:, : side * lanes].reshape(levels, 8, side, lanes).transpose(0, 2, 1, 3)
    return rows.reshape(levels * side * 8, lanes)[:count]


def body(
    tokens,
    norm_gain,
    router_weight,
    placement,
    expert_ids,
    w_gate,
    w_up,
    w_down,
    shared_gate,
    shared_up,
    shared_down,
):
    slots = placement.shape[0]
    tok_rows, width = tokens.shape
    capacity = 3 * tok_rows * expert_ids.shape[1] // (2 * slots)
    node_count = lax.axis_size("node")
    local_count = lax.axis_size("local")
    cores = node_count * local_count // slots
    x_count = local_count // cores
    y_count = math.gcd(node_count, x_count)
    dims = {"z": node_count // y_count, "y": y_count, "x": x_count, "c": cores}
    own_slot = lax.axis_index(AXES) // cores
    stride = {"x": 1, "y": x_count}

    def slices_of(*weights):
        slices = [weights]
        for step in range(1, cores):
            slices.append([shift(w, dims, "c", step) for w in weights])
        return slices

    with jax.named_scope("swap"):
        expert_slices = slices_of(w_gate, w_up, w_down)
        shared_slices = slices_of(shared_gate, shared_up, shared_down)

    floats = tokens.astype(F32)
    normed = (
        floats * lax.rsqrt(jnp.mean(floats * floats, -1, keepdims=True) + 1e-06) * norm_gain
    ).astype(BF16)
    routing = routing_rows(normed, router_weight, placement, expert_ids)
    block = jnp.concatenate([normed, pack(routing, width)], 0)

    place_iota = jnp.arange(1, capacity + 1, dtype=jnp.int32).astype(F32)[:, None]

    def chunk(block, step, first, second):
        with jax.named_scope(f"gather{step}"):
            blocks = [block] + [shift(block, dims, first, d) for d in range(1, dims[first])]
        place = own_slot // stride[second] % dims[second]
        chosen = []
        rows = [[b[:tok_rows] for b in blocks]]
        tables = [unpack(b[tok_rows:], 2 * slots, tok_rows).astype(F32) for b in blocks]
        for d in range(dims[second]):
            slot = own_slot + ((place + d) % dims[second] - place) * stride[second]
            pairs = []
            for table in tables:
                gates = lax.dynamic_slice_in_dim(table, slot, 1, 0)
                places = lax.dynamic_slice_in_dim(table, slots + slot, 1, 0)
                hot = places == place_iota
                pairs.append((hot.astype(BF16), jnp.where(hot, gates, 0.0).astype(BF16)))
            chosen.append(pairs)
        sent = []
        for pairs in chosen:
            sent.append(
                jnp.concatenate(
                    [
                        jnp.dot(hot, b[:tok_rows], preferred_element_type=F32).astype(BF16)
                        for (hot, _), b in zip(pairs, blocks)
                    ],
                    0,
                )
            )
        with jax.named_scope(f"out{step}"):
            came = [sent[0]] + [shift(sent[d], dims, second, d) for d in range(1, dims[second])]
        results = [feed_forward(r, expert_slices).astype(BF16) for r in came]
        with jax.named_scope(f"back{step}"):
            back = [results[0]] + [
                shift(results[d], dims, second, -d) for d in range(1, dims[second])
            ]
        parts = []
        for i in range(len(blocks)):
            weights = jnp.concatenate([pairs[i][1] for pairs in chosen], 0)
            values = jnp.concatenate([r[i * capacity : (i + 1) * capacity] for r in back], 0)
            parts.append(
                lax.dot_general(
                    weights, values, (((0,), (0,)), ((), ())), preferred_element_type=F32
                )
            )
        if step == 0:
            shared = feed_forward(
                jnp.concatenate([b[:tok_rows] for b in blocks], 0), shared_slices
            )
            parts = [p + shared[i * tok_rows : (i + 1) * tok_rows] for i, p in enumerate(parts)]
        total = parts[0]
        with jax.named_scope(f"reduce{step}"):
            for d in range(1, dims[first]):
                total = total + shift(parts[d].astype(BF16), dims, first, -d).astype(F32)
        return total

    totals = []
    for step in range(dims["z"]):
        if step:
            with jax.named_scope(f"ring{step}"):
                block = shift(block, dims, "z", 1)
        totals.append(chunk(block, step, *ORDERS[step % len(ORDERS)]))
    passed = None
    for step in range(1, dims["z"]):
        held = totals[step] if passed is None else totals[step] + passed
        with jax.named_scope(f"collect{step}"):
            passed = shift(held.astype(BF16), dims, "z", 1).astype(F32)
    out = totals[0] if passed is None else totals[0] + passed
    return out.astype(BF16)


def solution(mesh):
    in_specs = (
        P(AXES, None),
        P(),
        P(),
        P(),
        P(AXES, None),
        P(None, AXES),
        P(None, AXES),
        P(AXES, None),
        P(None, "local"),
        P(None, "local"),
        P("local", None),
    )
    out_specs = P(AXES, None)
    return jax.shard_map(body, mesh=mesh, in_specs=in_specs, out_specs=out_specs, check_vma=False)
```

```python
import math

import jax
import jax.numpy as jnp
import numpy as np
from jax import lax
from jax.experimental import pallas as pl
from jax.experimental.pallas import tpu as pltpu
from jax.sharding import PartitionSpec as P

AXES = ("node", "local")
F32 = jnp.float32
BF16 = jnp.bfloat16
STRIP = 8
UNUSED = -4096.0
PIECE = 256


def places(dims):
    return [dict(zip(dims, p)) for p in np.ndindex(*dims.values())]


def index_of(dims, place):
    index = 0
    for name, size in dims.items():
        index = index * size + place[name] % size
    return index


def moved(dims, place, axes, step):
    axis = axes[place["c"] % len(axes)]
    return index_of(dims, {**place, axis: place[axis] + step})


def shift(block, dims, axes, step):
    route = [(i, moved(dims, p, axes, step)) for i, p in enumerate(places(dims))]
    return lax.ppermute(block, AXES, route)


def targets(dims, axes):
    size = dims[axes[0]]
    table = [[moved(dims, p, axes, d) // dims["c"] for d in range(size)] for p in places(dims)]
    return lax.dynamic_index_in_dim(
        jnp.asarray(np.array(table, np.int32)), lax.axis_index(AXES), 0, keepdims=False
    )


def routing_rows(normed, router_weight, placement, expert_ids):
    slots = placement.shape[0]
    tok_rows = normed.shape[0]
    slot_iota = jnp.arange(slots, dtype=jnp.int32)
    to_slot = (placement[:, None] == slot_iota).astype(BF16)
    slot_router = jnp.dot(router_weight, to_slot, preferred_element_type=F32).astype(BF16)
    logits = lax.dot_general(slot_router, normed, (((0,), (1,)), ((), ())), preferred_element_type=F32)
    named = expert_ids[:, :, None] == slot_iota
    token_slots = jnp.sum(jnp.where(named, placement, 0), -1)
    hot = jnp.any(token_slots.T[:, None, :] == slot_iota[:, None], 0)
    picked = jnp.where(hot, jax.nn.sigmoid(logits), 0.0)
    gates = picked / jnp.sum(picked, 0, keepdims=True)
    upper = jnp.arange(tok_rows)[:, None] <= jnp.arange(tok_rows)
    running = jnp.dot(hot.astype(BF16), upper.astype(BF16), preferred_element_type=F32)
    return jnp.concatenate([gates, jnp.where(hot, running, UNUSED)], 0).astype(BF16)


def pack(rows, width):
    count, lanes = rows.shape
    strips = -(-count // STRIP)
    rows = jnp.pad(rows, ((0, strips * STRIP - count), (0, 0)))
    parts = [rows[i * STRIP : (i + 1) * STRIP] for i in range(strips)]
    packed = jnp.concatenate(parts, 1)
    return jnp.pad(packed, ((0, 0), (0, width - strips * lanes)))


def table_row(block, tok_rows, row):
    start = pl.multiple_of(row // STRIP * tok_rows, tok_rows)
    group = block[tok_rows : tok_rows + STRIP, pl.ds(start, tok_rows)].astype(F32)
    lines = lax.broadcasted_iota(jnp.int32, group.shape, 0)
    return jnp.sum(jnp.where(lines == row % STRIP, group, 0.0), 0, keepdims=True)


def choice(blocks, tok_rows, slots, slot, list_rows, capacity, gated):
    lines = lax.broadcasted_iota(jnp.int32, (list_rows, tok_rows), 0).astype(F32)
    columns = []
    for i, block in enumerate(blocks):
        place = table_row(block, tok_rows, slots + slot)
        value = table_row(block, tok_rows, slot) if gated else 1.0
        columns.append(jnp.where(lines + float(1 - i * capacity) == place, value, 0.0))
    return jnp.concatenate(columns, 1).astype(BF16)


def stacked(blocks, tok_rows):
    return jnp.concatenate([b[:tok_rows] for b in blocks], 0)


def vmem():
    return pl.BlockSpec(memory_space=pltpu.VMEM)


def anywhere():
    return pl.BlockSpec(memory_space=pl.ANY)


def send_rows(blocks, chosen, shape, after):
    slots, tok_rows, capacity, list_rows = shape
    width = blocks[0].shape[1]
    outs = chosen.shape[0] - 1

    def kernel(slot_ref, *refs):
        block_refs = refs[: len(blocks)]
        out_refs = refs[len(refs) - outs :]
        tokens = stacked(block_refs, tok_rows)
        for d, out in enumerate(out_refs):
            hot = choice(block_refs, tok_rows, slots, slot_ref[d + 1], list_rows, capacity, False)
            out[...] = jnp.dot(hot, tokens, preferred_element_type=F32).astype(BF16)

    flops = 2 * outs * list_rows * len(blocks) * tok_rows * width
    call = pl.pallas_call(
        kernel,
        out_shape=[jax.ShapeDtypeStruct((list_rows, width), BF16)] * outs,
        in_specs=[pl.BlockSpec(memory_space=pltpu.SMEM)]
        + [vmem()] * len(blocks)
        + [anywhere()] * len(after),
        out_specs=[vmem()] * outs,
        cost_estimate=pl.CostEstimate(flops=4 * flops, bytes_accessed=0, transcendentals=0),
        name="send_rows",
    )
    return list(call(chosen, *blocks, *after))


def feed_forward(blocks, came, slices, chosen, shape, after):
    slots, tok_rows, capacity, list_rows = shape
    width = blocks[0].shape[1]
    routed = chosen is not None
    group = list_rows if routed else len(blocks) * tok_rows
    groups = len(came) + 1
    count = group * groups
    hidden = slices[0][0].shape[0]
    pieces = [(lo, min(PIECE, hidden - lo)) for lo in range(0, hidden, PIECE)]
    result = BF16 if routed else F32

    def kernel(*refs):
        refs = list(refs)
        slot_ref = refs.pop(0) if routed else None
        block_refs = [refs.pop(0) for _ in blocks]
        came_refs = [refs.pop(0) for _ in came]
        weights = [[refs.pop(0) for _ in range(3)] for _ in slices]
        for _ in after:
            refs.pop(0)
        out_refs = [refs.pop(0) for _ in range(groups)]
        rows, active, total, gate_mem, up_mem, down_mem, sems = refs

        def copies(i, source, j):
            lo, size = pieces[j]
            part = pl.ds(lo, size)
            return [
                pltpu.make_async_copy(source[0].at[part], gate_mem.at[i, part], sems.at[i, 2 * j]),
                pltpu.make_async_copy(source[1].at[part], up_mem.at[i, part], sems.at[i, 2 * j + 1]),
            ]

        def down_copy(i, source):
            return pltpu.make_async_copy(source[2], down_mem.at[i], sems.at[i, 2 * len(pieces)])

        for i, source in enumerate(weights):
            for j in range(len(pieces)):
                for copy in copies(i, source, j):
                    copy.start()
            down_copy(i, source).start()

        tokens = stacked(block_refs, tok_rows)
        if routed:
            hot = choice(block_refs, tok_rows, slots, slot_ref[0], list_rows, capacity, False)
            rows[:group] = jnp.dot(hot, tokens, preferred_element_type=F32).astype(BF16)
        else:
            rows[:group] = tokens
        for d, ref in enumerate(came_refs):
            rows[(d + 1) * group : (d + 2) * group] = ref[...]
        total[...] = jnp.zeros_like(total)

        def one_slice(i, carry):
            values = rows[...]
            across = (((1,), (1,)), ((), ()))
            for j, (lo, size) in enumerate(pieces):
                for copy in copies(i, weights[0], j):
                    copy.wait()
                gate = lax.dot_general(
                    values, gate_mem[i, lo : lo + size], across, preferred_element_type=F32
                )
                up = lax.dot_general(
                    values, up_mem[i, lo : lo + size], across, preferred_element_type=F32
                )
                active[:, lo : lo + size] = (gate / (1.0 + jnp.exp(-gate)) * up).astype(BF16)
            down_copy(i, weights[0]).wait()
            total[...] += jnp.dot(active[...], down_mem[i], preferred_element_type=F32)
            return carry

        lax.fori_loop(0, len(slices), one_slice, 0)
        for d, out in enumerate(out_refs):
            out[...] = total[d * group : (d + 1) * group].astype(result)

    flops = 6 * count * width * hidden * len(slices)
    operands = [chosen] if routed else []
    call = pl.pallas_call(
        kernel,
        out_shape=[jax.ShapeDtypeStruct((group, width), result)] * groups,
        in_specs=[pl.BlockSpec(memory_space=pltpu.SMEM)] * len(operands)
        + [vmem()] * (len(blocks) + len(came))
        + [anywhere()] * (3 * len(slices) + len(after)),
        out_specs=[vmem()] * groups,
        scratch_shapes=[
            pltpu.VMEM((count, width), BF16),
            pltpu.VMEM((count, hidden), BF16),
            pltpu.VMEM((count, width), F32),
        ]
        + [pltpu.VMEM((len(slices), hidden, width), BF16)] * 3
        + [pltpu.SemaphoreType.DMA((len(slices), 2 * len(pieces) + 1))],
        cost_estimate=pl.CostEstimate(flops=flops, bytes_accessed=0, transcendentals=0),
        name="experts" if routed else "shared",
    )
    return list(call(*operands, *blocks, *came, *[w for s in slices for w in s], *after))


def combine(blocks, back, chosen, extra, shape, after):
    slots, tok_rows, capacity, list_rows = shape
    width = blocks[0].shape[1]

    def kernel(slot_ref, *refs):
        refs = list(refs)
        block_refs = [refs.pop(0) for _ in blocks]
        back_refs = [refs.pop(0) for _ in back]
        extra_refs = [refs.pop(0) for _ in extra]
        for _ in after:
            refs.pop(0)
        out_refs = refs
        weights = [
            choice(block_refs, tok_rows, slots, slot_ref[d], list_rows, capacity, True)
            for d in range(len(back))
        ]
        for i, out in enumerate(out_refs):
            span = slice(i * tok_rows, (i + 1) * tok_rows)
            sums = None
            for w, ref in zip(weights, back_refs):
                part = lax.dot_general(
                    w[:, span], ref[...], (((0,), (0,)), ((), ())), preferred_element_type=F32
                )
                sums = part if sums is None else sums + part
            for ref in extra_refs:
                sums = sums + ref[span]
            out[...] = sums.astype(out.dtype)

    flops = 2 * len(back) * list_rows * len(blocks) * tok_rows * width
    call = pl.pallas_call(
        kernel,
        out_shape=[
            jax.ShapeDtypeStruct((tok_rows, width), BF16 if i else F32) for i in range(len(blocks))
        ],
        in_specs=[pl.BlockSpec(memory_space=pltpu.SMEM)]
        + [vmem()] * (len(blocks) + len(back) + len(extra))
        + [anywhere()] * len(after),
        out_specs=[vmem()] * len(blocks),
        cost_estimate=pl.CostEstimate(flops=4 * flops, bytes_accessed=0, transcendentals=0),
        name="combine",
    )
    return list(call(chosen, *blocks, *back, *extra, *after))


def body(
    tokens,
    norm_gain,
    router_weight,
    placement,
    expert_ids,
    w_gate,
    w_up,
    w_down,
    shared_gate,
    shared_up,
    shared_down,
):
    slots = placement.shape[0]
    tok_rows, width = tokens.shape
    capacity = 3 * tok_rows * expert_ids.shape[1] // (2 * slots)
    node_count = lax.axis_size("node")
    local_count = lax.axis_size("local")
    cores = node_count * local_count // slots
    x_count = local_count // cores
    y_count = math.gcd(node_count, x_count)
    dims = {"z": node_count // y_count, "y": y_count, "x": x_count, "c": cores}
    list_rows = -(-x_count * capacity // 16) * 16
    shape = (slots, tok_rows, capacity, list_rows)
    steps = dims["z"]
    mixed = ("xy", "yx") if x_count == y_count else ("xy", "xy")
    orders = [("xy", "xy")] + [mixed] * (steps - 1)

    def slices_of(*weights):
        return [list(weights)] + [
            [shift(w, dims, "c", step) for w in weights] for step in range(1, cores)
        ]

    with jax.named_scope("swap_shared"):
        shared_slices = slices_of(shared_gate.T, shared_up.T, shared_down)
    with jax.named_scope("swap"):
        expert_slices = slices_of(w_gate.T, w_up.T, w_down)

    floats = tokens.astype(F32)
    normed = (
        floats * lax.rsqrt(jnp.mean(floats * floats, -1, keepdims=True) + 1e-06) * norm_gain
    ).astype(BF16)
    routing = routing_rows(normed, router_weight, placement, expert_ids)
    own = [jnp.concatenate([normed, pack(routing, width)], 0)]
    for step in range(1, steps):
        with jax.named_scope(f"ring{step}"):
            own.append(shift(own[-1], dims, "z", 1))

    last = []
    blocks, chosen, came, results, parts = {}, {}, {}, {}, {}
    firsts = [[o[0] for o in order] for order in orders]
    seconds = [[o[1] for o in order] for order in orders]
    for step in range(steps):
        chosen[step] = targets(dims, seconds[step])
        with jax.named_scope(f"gather{step}"):
            blocks[step] = [own[step]] + [
                shift(own[step], dims, firsts[step], d) for d in range(1, dims[firsts[step][0]])
            ]

    def send(step):
        nonlocal last
        sent = send_rows(blocks[step], chosen[step], shape, last)
        last = sent[:1]
        with jax.named_scope(f"out{step}"):
            came[step] = [shift(r, dims, seconds[step], d + 1) for d, r in enumerate(sent)]

    def run(step):
        nonlocal last
        out = feed_forward(blocks[step], came[step], expert_slices, chosen[step], shape, last)
        last = out[:1]
        with jax.named_scope(f"back{step}"):
            results[step] = out[:1] + [
                shift(r, dims, seconds[step], -d - 1) for d, r in enumerate(out[1:])
            ]

    def join(step, extra=()):
        nonlocal last
        out = combine(blocks[step], results[step], chosen[step], extra, shape, last)
        last = out[:1]
        with jax.named_scope(f"reduce{step}"):
            parts[step] = out[:1] + [
                shift(r, dims, firsts[step], -d - 1) for d, r in enumerate(out[1:])
            ]

    later = list(range(1, steps))
    send(0)
    shared = feed_forward(blocks[0], [], shared_slices, None, shape, last)
    last = shared[:1]
    for step in later[:2]:
        send(step)
    for n, step in enumerate(later):
        run(step)
        if n + 2 < len(later):
            send(later[n + 2])
        if n > 0:
            join(later[n - 1])
    run(0)
    for step in later[-1:]:
        join(step)
    join(0, shared)

    passed = []
    for step in later + [0]:
        total = parts[step][0]
        for part in parts[step][1:] + passed:
            total = total + part.astype(F32)
        total = total.astype(BF16)
        if step:
            with jax.named_scope(f"collect{step}"):
                passed = [shift(total, dims, "z", 1)]
    return total


def solution(mesh):
    in_specs = (
        P(AXES, None),
        P(),
        P(),
        P(),
        P(AXES, None),
        P(None, AXES),
        P(None, AXES),
        P(AXES, None),
        P(None, "local"),
        P(None, "local"),
        P("local", None),
    )
    out_specs = P(AXES, None)
    return jax.shard_map(body, mesh=mesh, in_specs=in_specs, out_specs=out_specs, check_vma=False)
```

```python
import math

import jax
import jax.numpy as jnp
import numpy as np
from jax import lax
from jax.experimental import pallas as pl
from jax.experimental.pallas import tpu as pltpu
from jax.sharding import PartitionSpec as P


AXES = ("node", "local")
F32 = jnp.float32
BF16 = jnp.bfloat16
STRIP = 8
UNUSED = -4096.0
PIECE = 256
LIMIT = 16 << 20


def places(dims):
    return [dict(zip(dims, p)) for p in np.ndindex(*dims.values())]


def index_of(dims, place):
    index = 0
    for name, size in dims.items():
        index = index * size + place[name] % size
    return index


def moved(dims, place, axes, step):
    axis = axes[place["c"] % len(axes)]
    return index_of(dims, {**place, axis: place[axis] + step})


def shift(block, dims, axes, step):
    route = [(i, moved(dims, p, axes, step)) for i, p in enumerate(places(dims))]
    return lax.ppermute(block, AXES, route)


def targets(dims, axes):
    size = dims[axes[0]]
    table = [[moved(dims, p, axes, d) // dims["c"] for d in range(size)] for p in places(dims)]
    return lax.dynamic_index_in_dim(
        jnp.asarray(np.array(table, np.int32)), lax.axis_index(AXES), 0, keepdims=False
    )


def routing_rows(normed, router_weight, placement, expert_ids):
    slots = placement.shape[0]
    tok_rows = normed.shape[0]
    slot_iota = jnp.arange(slots, dtype=jnp.int32)
    to_slot = (placement[:, None] == slot_iota).astype(BF16)
    slot_router = jnp.dot(router_weight, to_slot, preferred_element_type=F32).astype(BF16)
    logits = lax.dot_general(slot_router, normed, (((0,), (1,)), ((), ())), preferred_element_type=F32)
    named = expert_ids[:, :, None] == slot_iota
    token_slots = jnp.sum(jnp.where(named, placement, 0), -1)
    hot = jnp.any(token_slots.T[:, None, :] == slot_iota[:, None], 0)
    picked = jnp.where(hot, jax.nn.sigmoid(logits), 0.0)
    gates = picked / jnp.sum(picked, 0, keepdims=True)
    upper = jnp.arange(tok_rows)[:, None] <= jnp.arange(tok_rows)
    running = jnp.dot(hot.astype(BF16), upper.astype(BF16), preferred_element_type=F32)
    return jnp.concatenate([gates, jnp.where(hot, running, UNUSED)], 0).astype(BF16)


def pack(rows, width):
    count, lanes = rows.shape
    strips = -(-count // STRIP)
    rows = jnp.pad(rows, ((0, strips * STRIP - count), (0, 0)))
    parts = [rows[i * STRIP : (i + 1) * STRIP] for i in range(strips)]
    packed = jnp.concatenate(parts, 1)
    return jnp.pad(packed, ((0, 0), (0, width - strips * lanes)))


def table_row(block, tok_rows, row):
    start = pl.multiple_of(row // STRIP * tok_rows, tok_rows)
    group = block[tok_rows : tok_rows + STRIP, pl.ds(start, tok_rows)].astype(F32)
    lines = lax.broadcasted_iota(jnp.int32, group.shape, 0)
    return jnp.sum(jnp.where(lines == row % STRIP, group, 0.0), 0, keepdims=True)


def choice(blocks, tok_rows, slots, slot, list_rows, capacity, gated):
    lines = lax.broadcasted_iota(jnp.int32, (list_rows, tok_rows), 0).astype(F32)
    columns = []
    for i, block in enumerate(blocks):
        place = table_row(block, tok_rows, slots + slot)
        value = table_row(block, tok_rows, slot) if gated else 1.0
        columns.append(jnp.where(lines + float(1 - i * capacity) == place, value, 0.0))
    return jnp.concatenate(columns, 1).astype(BF16)


def stacked(blocks, tok_rows):
    return jnp.concatenate([b[:tok_rows] for b in blocks], 0)


def vmem():
    return pl.BlockSpec(memory_space=pltpu.VMEM)


def kept(arrays, space=pltpu.VMEM):
    return [pltpu.with_memory_space_constraint(a, space) for a in arrays]


def load(arrays, after):
    def kernel(*refs):
        sources, outs, sems = refs[: len(arrays)], refs[-len(arrays) - 1 : -1], refs[-1]
        copies = [pltpu.make_async_copy(s, o, sems.at[i]) for i, (s, o) in enumerate(zip(sources, outs))]
        for copy in copies:
            copy.start()
        for copy in copies:
            copy.wait()

    call = pl.pallas_call(
        kernel,
        out_shape=[pltpu.VMEM(a.shape, a.dtype) for a in arrays],
        in_specs=[anywhere()] * (len(arrays) + len(after)),
        out_specs=[vmem()] * len(arrays),
        scratch_shapes=[pltpu.SemaphoreType.DMA((len(arrays),))],
        compiler_params=pltpu.CompilerParams(vmem_limit_bytes=LIMIT),
        cost_estimate=pl.CostEstimate(flops=1 << 32, bytes_accessed=0, transcendentals=0),
        name="load",
    )
    return list(call(*kept(arrays, pltpu.HBM), *after))


def anywhere():
    return pl.BlockSpec(memory_space=pl.ANY)


def send_rows(blocks, chosen, shape, after):
    slots, tok_rows, capacity, list_rows = shape
    width = blocks[0].shape[1]
    outs = chosen.shape[0] - 1

    def kernel(slot_ref, *refs):
        block_refs = refs[: len(blocks)]
        out_refs = refs[len(refs) - outs :]
        tokens = stacked(block_refs, tok_rows)
        for d, out in enumerate(out_refs):
            hot = choice(block_refs, tok_rows, slots, slot_ref[d + 1], list_rows, capacity, False)
            out[...] = jnp.dot(hot, tokens, preferred_element_type=F32).astype(BF16)

    flops = 2 * outs * list_rows * len(blocks) * tok_rows * width
    call = pl.pallas_call(
        kernel,
        out_shape=[pltpu.VMEM((list_rows, width), BF16)] * outs,
        in_specs=[pl.BlockSpec(memory_space=pltpu.SMEM)]
        + [vmem()] * len(blocks)
        + [anywhere()] * len(after),
        out_specs=[vmem()] * outs,
        cost_estimate=pl.CostEstimate(flops=4 * flops, bytes_accessed=0, transcendentals=0),
        compiler_params=pltpu.CompilerParams(vmem_limit_bytes=LIMIT),
        name="send_rows",
    )
    return list(call(chosen, *kept(blocks), *after))


def feed_forward(blocks, came, slices, chosen, shape, after):
    slots, tok_rows, capacity, list_rows = shape
    width = blocks[0].shape[1]
    routed = chosen is not None
    group = list_rows if routed else len(blocks) * tok_rows
    groups = 1 + (len(came) if routed else len(came) // len(blocks))
    count = group * groups
    hidden = slices[0][0].shape[0]
    pieces = [(lo, min(PIECE, hidden - lo)) for lo in range(0, hidden, PIECE)]

    def kernel(*refs):
        refs = list(refs)
        slot_ref = refs.pop(0) if routed else None
        block_refs = [refs.pop(0) for _ in blocks]
        came_refs = [refs.pop(0) for _ in came]
        weights = [[refs.pop(0) for _ in range(3)] for _ in slices]
        for _ in after:
            refs.pop(0)
        out_refs = [refs.pop(0) for _ in range(groups)]
        rows, active, total, *streamed = refs
        if not routed:
            *stores, sems = streamed

            def copy(i, n, j, part):
                source, store = weights[i][n].at[part], stores[n].at[i, part]
                return pltpu.make_async_copy(source, store, sems.at[i, n, j])

            parts = [pl.ds(lo, size) for lo, size in pieces]
            for i in range(len(slices)):
                for j, part in enumerate(parts):
                    copy(i, 0, j, part).start()
                    copy(i, 1, j, part).start()
                copy(i, 2, 0, pl.ds(0, hidden)).start()

        tokens = stacked(block_refs, tok_rows)
        if routed:
            hot = choice(block_refs, tok_rows, slots, slot_ref[0], list_rows, capacity, False)
            rows[:group] = jnp.dot(hot, tokens, preferred_element_type=F32).astype(BF16)
        else:
            rows[:group] = tokens
        if routed:
            for d, ref in enumerate(came_refs):
                rows[(d + 1) * group : (d + 2) * group] = ref[...]
        else:
            for d, ref in enumerate(came_refs):
                start = group + d * tok_rows
                rows[start : start + tok_rows] = ref[:tok_rows]
        across = (((1,), (1,)), ((), ()))
        for i, (gate_ref, up_ref, down_ref) in enumerate(weights):
            values = rows[...]
            if not routed:
                gate_ref, up_ref, down_ref = [store.at[i] for store in stores]
            for j, (lo, size) in enumerate(pieces):
                span = slice(lo, lo + size)
                if not routed:
                    copy(i, 0, j, parts[j]).wait()
                    copy(i, 1, j, parts[j]).wait()
                gate = lax.dot_general(values, gate_ref[span], across, preferred_element_type=F32)
                up = lax.dot_general(values, up_ref[span], across, preferred_element_type=F32)
                active[:, span] = (gate / (1.0 + jnp.exp(-gate)) * up).astype(BF16)
            if not routed:
                copy(i, 2, 0, pl.ds(0, hidden)).wait()
            part = jnp.dot(active[...], down_ref[...], preferred_element_type=F32)
            if i:
                part = total[...] + part
            if i + 1 < len(weights):
                total[...] = part
                continue
            for d, out in enumerate(out_refs):
                out[...] = part[d * group : (d + 1) * group].astype(out.dtype)

    flops = 6 * count * width * hidden * len(slices)
    operands = [chosen] if routed else []
    stream = []
    if not routed:
        stream = [pltpu.VMEM((len(slices), hidden, width), BF16)] * 3
        stream += [pltpu.SemaphoreType.DMA((len(slices), 3, len(pieces)))]
    call = pl.pallas_call(
        kernel,
        out_shape=[
            pltpu.VMEM((group, width), BF16 if routed or d else F32) for d in range(groups)
        ],
        in_specs=[pl.BlockSpec(memory_space=pltpu.SMEM)] * len(operands)
        + [vmem()] * (len(blocks) + len(came))
        + [vmem() if routed else anywhere()] * (3 * len(slices))
        + [anywhere()] * len(after),
        out_specs=[vmem()] * groups,
        scratch_shapes=[
            pltpu.VMEM((count, width), BF16),
            pltpu.VMEM((count, hidden), BF16),
            pltpu.VMEM((count, width), F32),
        ]
        + stream,
        compiler_params=pltpu.CompilerParams(vmem_limit_bytes=LIMIT if routed else 2 * LIMIT),
        cost_estimate=pl.CostEstimate(flops=flops, bytes_accessed=0, transcendentals=0),
        name="experts" if routed else "shared",
    )
    weights = [w for s in slices for w in s]
    weights = kept(weights, pltpu.VMEM if routed else pltpu.HBM)
    return list(call(*operands, *kept(blocks), *kept(came), *weights, *after))


def combine(blocks, back, chosen, extra, shape, after):
    slots, tok_rows, capacity, list_rows = shape
    width = blocks[0].shape[1]

    def kernel(slot_ref, *refs):
        refs = list(refs)
        block_refs = [refs.pop(0) for _ in blocks]
        back_refs = [refs.pop(0) for _ in back]
        extra_refs = [refs.pop(0) for _ in extra]
        for _ in after:
            refs.pop(0)
        out_refs = refs
        weights = [
            choice(block_refs, tok_rows, slots, slot_ref[d], list_rows, capacity, True)
            for d in range(len(back))
        ]
        for i, out in enumerate(out_refs):
            span = slice(i * tok_rows, (i + 1) * tok_rows)
            sums = None
            for w, ref in zip(weights, back_refs):
                part = lax.dot_general(
                    w[:, span], ref[...], (((0,), (0,)), ((), ())), preferred_element_type=F32
                )
                sums = part if sums is None else sums + part
            for ref in extra_refs:
                sums = sums + ref[span]
            out[...] = sums.astype(out.dtype)

    flops = 2 * len(back) * list_rows * len(blocks) * tok_rows * width
    call = pl.pallas_call(
        kernel,
        out_shape=[
            pltpu.VMEM((tok_rows, width), BF16 if i else F32) for i in range(len(blocks))
        ],
        in_specs=[pl.BlockSpec(memory_space=pltpu.SMEM)]
        + [vmem()] * (len(blocks) + len(back) + len(extra))
        + [anywhere()] * len(after),
        out_specs=[vmem()] * len(blocks),
        cost_estimate=pl.CostEstimate(flops=4 * flops, bytes_accessed=0, transcendentals=0),
        compiler_params=pltpu.CompilerParams(vmem_limit_bytes=LIMIT),
        name="combine",
    )
    return list(call(chosen, *kept(blocks), *kept(back), *kept(extra), *after))


def body(
    tokens,
    norm_gain,
    router_weight,
    placement,
    expert_ids,
    w_gate,
    w_up,
    w_down,
    shared_gate,
    shared_up,
    shared_down,
):
    slots = placement.shape[0]
    tok_rows, width = tokens.shape
    capacity = 3 * tok_rows * expert_ids.shape[1] // (2 * slots)
    node_count = lax.axis_size("node")
    local_count = lax.axis_size("local")
    cores = node_count * local_count // slots
    x_count = local_count // cores
    y_count = math.gcd(node_count, x_count)
    dims = {"z": node_count // y_count, "y": y_count, "x": x_count, "c": cores}
    list_rows = -(-x_count * capacity // 16) * 16
    shape = (slots, tok_rows, capacity, list_rows)
    steps = dims["z"]
    mixed = ("xy", "yx") if x_count == y_count else ("xy", "xy")
    orders = [("xy", "xy")] + [mixed] * (steps - 1)

    def slices_of(*weights):
        return [list(weights)] + [
            [shift(w, dims, "c", step) for w in weights] for step in range(1, cores)
        ]

    expert_slices = slices_of(w_gate.T, w_up.T, w_down)

    floats = tokens.astype(F32)
    normed = (
        floats * lax.rsqrt(jnp.mean(floats * floats, -1, keepdims=True) + 1e-06) * norm_gain
    ).astype(BF16)
    routing = routing_rows(normed, router_weight, placement, expert_ids)
    own = [jnp.concatenate([normed, pack(routing, width)], 0)]
    for _ in range(1, steps):
        own.append(shift(own[-1], dims, "z", 1))

    last = own[:1]
    loaded = load([w for weights in expert_slices for w in weights], last)
    expert_slices = [loaded[i : i + 3] for i in range(0, len(loaded), 3)]
    last = loaded[-1:]
    blocks, chosen, came, results, parts = {}, {}, {}, {}, {}
    firsts = [[o[0] for o in order] for order in orders]
    seconds = [[o[1] for o in order] for order in orders]
    for step in range(steps):
        chosen[step] = targets(dims, seconds[step])
        blocks[step] = [own[step]] + [
            shift(own[step], dims, firsts[step], d) for d in range(1, dims[firsts[step][0]])
        ]

    def send(step):
        nonlocal last
        sent = send_rows(blocks[step], chosen[step], shape, last)
        last = sent[:1]
        came[step] = [shift(r, dims, seconds[step], d + 1) for d, r in enumerate(sent)]

    def run(step):
        nonlocal last
        results[step] = feed_forward(
            blocks[step], came[step], expert_slices, chosen[step], shape, last
        )
        last = results[step][:1]

    def give(step, held=None):
        own_rows, *rest = results[step]
        if held is not None:
            rest = lax.optimization_barrier((*rest, results[held][0]))[:-1]
        results[step] = [own_rows] + [
            shift(r, dims, seconds[step], -d - 1) for d, r in enumerate(rest)
        ]

    def join(step, extra=()):
        nonlocal last
        out = combine(blocks[step], results[step], chosen[step], extra, shape, last)
        last = out[:1]
        parts[step] = out[:1] + [
            shift(r, dims, firsts[step], -d - 1) for d, r in enumerate(out[1:])
        ]

    later = list(range(1, steps))
    send(0)
    peers = [shift(b, dims, "c", d) for d in range(1, cores) for b in blocks[0]]
    shared = feed_forward(
        blocks[0], peers, [[shared_gate.T, shared_up.T, shared_down]], None, shape, last
    )
    last = shared[:1]
    shared = shared[:1] + [shift(r, dims, "c", -d - 1) for d, r in enumerate(shared[1:])]
    for step in later[:1]:
        send(step)
    run(0)
    for n, step in enumerate(later):
        if n + 1 < len(later):
            send(later[n + 1])
        if n > 1:
            join(later[n - 2])
        run(step)
        give(step)
        if n == 0:
            give(0, step)
    for step in later[-2:-1]:
        join(step)
    if not later:
        give(0)
    join(0, shared)
    for step in later[-1:]:
        join(step)

    passed = []
    for step in later + [0]:
        total = parts[step][0]
        for part in parts[step][1:] + passed:
            total = total + part.astype(F32)
        total = total.astype(BF16)
        if step:
            passed = [shift(total, dims, "z", 1)]
    return total


def solution(mesh):
    in_specs = (
        P(AXES, None),
        P(),
        P(),
        P(),
        P(AXES, None),
        P(None, AXES),
        P(None, AXES),
        P(AXES, None),
        P(None, "local"),
        P(None, "local"),
        P("local", None),
    )
    out_specs = P(AXES, None)

    return jax.shard_map(body, mesh=mesh, in_specs=in_specs, out_specs=out_specs, check_vma=False)
```

```python
import math

import jax
import jax.numpy as jnp
import numpy as np
from jax import lax
from jax.experimental import pallas as pl
from jax.experimental.pallas import tpu as pltpu
from jax.sharding import PartitionSpec as P


AXES = ("node", "local")
F32 = jnp.float32
BF16 = jnp.bfloat16
STRIP = 8
UNUSED = -4096.0
PIECE = 256
LIMIT = 10 << 20


def places(dims):
    return [dict(zip(dims, p)) for p in np.ndindex(*dims.values())]


def index_of(dims, place):
    index = 0
    for name, size in dims.items():
        index = index * size + place[name] % size
    return index


def moved(dims, place, axes, step):
    axis = axes[place["c"] % len(axes)]
    return index_of(dims, {**place, axis: place[axis] + step})


def shift(block, dims, axes, step, only=None):
    route = [
        (i, moved(dims, p, axes, step))
        for i, p in enumerate(places(dims))
        if only is None or p["c"] in only
    ]
    return lax.ppermute(block, AXES, route)


def targets(dims, axes, direct):
    size = dims[axes[0]]
    table = [
        [moved(dims, p, axes, d) // dims["c"] for d in range(size)] + [int(p["c"] in direct)]
        for p in places(dims)
    ]
    return lax.dynamic_index_in_dim(
        jnp.asarray(np.array(table, np.int32)), lax.axis_index(AXES), 0, keepdims=False
    )


def routing_rows(normed, router_weight, placement, expert_ids):
    slots = placement.shape[0]
    tok_rows = normed.shape[0]
    slot_iota = jnp.arange(slots, dtype=jnp.int32)
    to_slot = (placement[:, None] == slot_iota).astype(BF16)
    slot_router = jnp.dot(router_weight, to_slot, preferred_element_type=F32).astype(BF16)
    logits = lax.dot_general(slot_router, normed, (((0,), (1,)), ((), ())), preferred_element_type=F32)
    named = expert_ids[:, :, None] == slot_iota
    token_slots = jnp.sum(jnp.where(named, placement, 0), -1)
    hot = jnp.any(token_slots.T[:, None, :] == slot_iota[:, None], 0)
    picked = jnp.where(hot, jax.nn.sigmoid(logits), 0.0)
    gates = picked / jnp.sum(picked, 0, keepdims=True)
    upper = jnp.arange(tok_rows)[:, None] <= jnp.arange(tok_rows)
    running = jnp.dot(hot.astype(BF16), upper.astype(BF16), preferred_element_type=F32)
    return jnp.concatenate([gates, jnp.where(hot, running, UNUSED)], 0).astype(BF16)


def pack(rows, width):
    count, lanes = rows.shape
    strips = -(-count // STRIP)
    rows = jnp.pad(rows, ((0, strips * STRIP - count), (0, 0)))
    parts = [rows[i * STRIP : (i + 1) * STRIP] for i in range(strips)]
    packed = jnp.concatenate(parts, 1)
    return jnp.pad(packed, ((0, 0), (0, width - strips * lanes)))


def table_row(block, tok_rows, row):
    start = pl.multiple_of(row // STRIP * tok_rows, tok_rows)
    group = block[tok_rows : tok_rows + STRIP, pl.ds(start, tok_rows)].astype(F32)
    lines = lax.broadcasted_iota(jnp.int32, group.shape, 0)
    return jnp.sum(jnp.where(lines == row % STRIP, group, 0.0), 0, keepdims=True)


def choice(blocks, tok_rows, slots, slot, list_rows, capacity, gated):
    lines = lax.broadcasted_iota(jnp.int32, (list_rows, tok_rows), 0).astype(F32)
    columns = []
    for i, block in enumerate(blocks):
        place = table_row(block, tok_rows, slots + slot)
        value = table_row(block, tok_rows, slot) if gated else 1.0
        columns.append(jnp.where(lines + float(1 - i * capacity) == place, value, 0.0))
    return jnp.concatenate(columns, 1).astype(BF16)


def stacked(blocks, tok_rows):
    return jnp.concatenate([b[:tok_rows] for b in blocks], 0)


def vmem():
    return pl.BlockSpec(memory_space=pltpu.VMEM)


def kept(arrays, space=pltpu.VMEM):
    return [pltpu.with_memory_space_constraint(a, space) for a in arrays]


def load(arrays, after):
    def kernel(*refs):
        sources, outs, sems = refs[: len(arrays)], refs[-len(arrays) - 1 : -1], refs[-1]
        copies = [pltpu.make_async_copy(s, o, sems.at[i]) for i, (s, o) in enumerate(zip(sources, outs))]
        for copy in copies:
            copy.start()
        for copy in copies:
            copy.wait()

    call = pl.pallas_call(
        kernel,
        out_shape=[pltpu.VMEM(a.shape, a.dtype) for a in arrays],
        in_specs=[anywhere()] * (len(arrays) + len(after)),
        out_specs=[vmem()] * len(arrays),
        scratch_shapes=[pltpu.SemaphoreType.DMA((len(arrays),))],
        compiler_params=pltpu.CompilerParams(vmem_limit_bytes=LIMIT),
        cost_estimate=pl.CostEstimate(flops=1 << 32, bytes_accessed=0, transcendentals=0),
        name="load",
    )
    return list(call(*kept(arrays, pltpu.HBM), *after))


def anywhere():
    return pl.BlockSpec(memory_space=pl.ANY)


def send_rows(blocks, chosen, shape, after):
    slots, tok_rows, capacity, list_rows = shape
    width = blocks[0].shape[1]
    outs = chosen.shape[0] - 2

    def kernel(slot_ref, *refs):
        block_refs = refs[: len(blocks)]
        out_refs = refs[len(refs) - outs :]
        tokens = stacked(block_refs, tok_rows)
        for d, out in enumerate(out_refs):
            hot = choice(block_refs, tok_rows, slots, slot_ref[d + 1], list_rows, capacity, False)
            out[...] = jnp.dot(hot, tokens, preferred_element_type=F32).astype(BF16)

    flops = 2 * outs * list_rows * len(blocks) * tok_rows * width
    call = pl.pallas_call(
        kernel,
        out_shape=[pltpu.VMEM((list_rows, width), BF16)] * outs,
        in_specs=[pl.BlockSpec(memory_space=pltpu.SMEM)]
        + [vmem()] * len(blocks)
        + [anywhere()] * len(after),
        out_specs=[vmem()] * outs,
        cost_estimate=pl.CostEstimate(flops=4 * flops, bytes_accessed=0, transcendentals=0),
        compiler_params=pltpu.CompilerParams(vmem_limit_bytes=LIMIT),
        name="send_rows",
    )
    return list(call(chosen, *kept(blocks), *after))


def feed_forward(blocks, came, slices, chosen, shape, after):
    slots, tok_rows, capacity, list_rows = shape
    width = blocks[0].shape[1]
    routed = chosen is not None
    group = list_rows if routed else len(blocks) * tok_rows
    groups = 1 + (len(came) if routed else len(came) // len(blocks))
    count = group * groups
    hidden = slices[0][0].shape[0]
    pieces = [(lo, min(PIECE, hidden - lo)) for lo in range(0, hidden, PIECE)]

    def kernel(*refs):
        refs = list(refs)
        slot_ref = refs.pop(0) if routed else None
        block_refs = [refs.pop(0) for _ in blocks]
        came_refs = [refs.pop(0) for _ in came]
        weights = [[refs.pop(0) for _ in range(3)] for _ in slices]
        for _ in after:
            refs.pop(0)
        out_refs = [refs.pop(0) for _ in range(groups)]
        rows, active, total, *streamed = refs
        if not routed:
            *stores, sems = streamed

            def copy(i, n, j, part):
                source, store = weights[i][n].at[part], stores[n].at[i, part]
                return pltpu.make_async_copy(source, store, sems.at[i, n, j])

            parts = [pl.ds(lo, size) for lo, size in pieces]
            for i in range(len(slices)):
                for j, part in enumerate(parts):
                    copy(i, 0, j, part).start()
                    copy(i, 1, j, part).start()
                copy(i, 2, 0, pl.ds(0, hidden)).start()

        tokens = stacked(block_refs, tok_rows)
        if routed:
            hot = choice(block_refs, tok_rows, slots, slot_ref[0], list_rows, capacity, False)
            rows[:group] = jnp.dot(hot, tokens, preferred_element_type=F32).astype(BF16)
        else:
            rows[:group] = tokens
        if routed:
            for d, ref in enumerate(came_refs):
                rows[(d + 1) * group : (d + 2) * group] = ref[...]
        else:
            for d, ref in enumerate(came_refs):
                start = group + d * tok_rows
                rows[start : start + tok_rows] = ref[:tok_rows]
        across = (((1,), (1,)), ((), ()))
        for i, (gate_ref, up_ref, down_ref) in enumerate(weights):
            values = rows[...]
            if not routed:
                gate_ref, up_ref, down_ref = [store.at[i] for store in stores]
            for j, (lo, size) in enumerate(pieces):
                span = slice(lo, lo + size)
                if not routed:
                    copy(i, 0, j, parts[j]).wait()
                    copy(i, 1, j, parts[j]).wait()
                gate = lax.dot_general(values, gate_ref[span], across, preferred_element_type=F32)
                up = lax.dot_general(values, up_ref[span], across, preferred_element_type=F32)
                active[:, span] = (gate / (1.0 + jnp.exp(-gate)) * up).astype(BF16)
            if not routed:
                copy(i, 2, 0, pl.ds(0, hidden)).wait()
            part = jnp.dot(active[...], down_ref[...], preferred_element_type=F32)
            if i:
                part = total[...] + part
            if i + 1 < len(weights):
                total[...] = part
                continue
            for d, out in enumerate(out_refs):
                out[...] = part[d * group : (d + 1) * group].astype(out.dtype)

    flops = 6 * count * width * hidden * len(slices)
    operands = [chosen] if routed else []
    stream = []
    if not routed:
        stream = [pltpu.VMEM((len(slices), hidden, width), BF16)] * 3
        stream += [pltpu.SemaphoreType.DMA((len(slices), 3, len(pieces)))]
    call = pl.pallas_call(
        kernel,
        out_shape=[
            pltpu.VMEM((group, width), BF16 if routed or d else F32) for d in range(groups)
        ],
        in_specs=[pl.BlockSpec(memory_space=pltpu.SMEM)] * len(operands)
        + [vmem()] * (len(blocks) + len(came))
        + [vmem() if routed else anywhere()] * (3 * len(slices))
        + [anywhere()] * len(after),
        out_specs=[vmem()] * groups,
        scratch_shapes=[
            pltpu.VMEM((count, width), BF16),
            pltpu.VMEM((count, hidden), BF16),
            pltpu.VMEM((count, width), F32),
        ]
        + stream,
        compiler_params=pltpu.CompilerParams(vmem_limit_bytes=LIMIT if routed else 2 * LIMIT),
        cost_estimate=pl.CostEstimate(flops=flops, bytes_accessed=0, transcendentals=0),
        name="experts" if routed else "shared",
    )
    weights = [w for s in slices for w in s]
    weights = kept(weights, pltpu.VMEM if routed else pltpu.HBM)
    return list(call(*operands, *kept(blocks), *kept(came), *weights, *after))


def combine(blocks, back, chosen, extra, shape, after):
    slots, tok_rows, capacity, list_rows = shape
    width = blocks[0].shape[1]

    def kernel(slot_ref, *refs):
        refs = list(refs)
        block_refs = [refs.pop(0) for _ in blocks]
        back_refs = [refs.pop(0) for _ in back]
        extra_refs = [refs.pop(0) for _ in extra]
        for _ in after:
            refs.pop(0)
        out_refs = refs
        weights = [
            choice(block_refs, tok_rows, slots, slot_ref[d], list_rows, capacity, True)
            for d in range(len(back))
        ]
        for i, out in enumerate(out_refs):
            span = slice(i * tok_rows, (i + 1) * tok_rows)
            sums = None
            for w, ref in zip(weights, back_refs):
                part = lax.dot_general(
                    w[:, span], ref[...], (((0,), (0,)), ((), ())), preferred_element_type=F32
                )
                sums = part if sums is None else sums + part
            for ref in extra_refs:
                more = ref[span].astype(F32)
                sums = sums + (more * slot_ref[len(back)].astype(F32) if i else more)
            out[...] = sums.astype(out.dtype)

    flops = 2 * len(back) * list_rows * len(blocks) * tok_rows * width
    call = pl.pallas_call(
        kernel,
        out_shape=[
            pltpu.VMEM((tok_rows, width), BF16 if i else F32) for i in range(len(blocks))
        ],
        in_specs=[pl.BlockSpec(memory_space=pltpu.SMEM)]
        + [vmem()] * (len(blocks) + len(back) + len(extra))
        + [anywhere()] * len(after),
        out_specs=[vmem()] * len(blocks),
        cost_estimate=pl.CostEstimate(flops=4 * flops, bytes_accessed=0, transcendentals=0),
        compiler_params=pltpu.CompilerParams(vmem_limit_bytes=LIMIT),
        name="combine",
    )
    return list(call(chosen, *kept(blocks), *kept(back), *kept(extra), *after))


def body(
    tokens,
    norm_gain,
    router_weight,
    placement,
    expert_ids,
    w_gate,
    w_up,
    w_down,
    shared_gate,
    shared_up,
    shared_down,
):
    slots = placement.shape[0]
    tok_rows, width = tokens.shape
    capacity = 3 * tok_rows * expert_ids.shape[1] // (2 * slots)
    node_count = lax.axis_size("node")
    local_count = lax.axis_size("local")
    cores = node_count * local_count // slots
    x_count = local_count // cores
    y_count = math.gcd(node_count, x_count)
    dims = {"z": node_count // y_count, "y": y_count, "x": x_count, "c": cores}
    list_rows = -(-x_count * capacity // 16) * 16
    shape = (slots, tok_rows, capacity, list_rows)
    steps = dims["z"]
    mixed = ("xy", "yx") if x_count == y_count else ("xy", "xy")
    orders = [mixed] * steps
    direct = [c for c in range(cores) if mixed[c % 2][0] == "x"]
    others = [c for c in range(cores) if c not in direct]

    def slices_of(*weights):
        return [list(weights)] + [
            [shift(w, dims, "c", step) for w in weights] for step in range(1, cores)
        ]

    expert_slices = slices_of(w_gate.T, w_up.T, w_down)

    floats = tokens.astype(F32)
    normed = (
        floats * lax.rsqrt(jnp.mean(floats * floats, -1, keepdims=True) + 1e-06) * norm_gain
    ).astype(BF16)
    routing = routing_rows(normed, router_weight, placement, expert_ids)
    own = [jnp.concatenate([normed, pack(routing, width)], 0)]
    for _ in range(1, steps):
        own.append(shift(own[-1], dims, "z", 1))

    last = own[:1]
    blocks, chosen, came, results, parts = {}, {}, {}, {}, {}
    firsts = [[o[0] for o in order] for order in orders]
    seconds = [[o[1] for o in order] for order in orders]
    for step in range(steps):
        chosen[step] = targets(dims, seconds[step], direct)
        blocks[step] = [own[step]] + [
            shift(own[step], dims, firsts[step], d) for d in range(1, dims[firsts[step][0]])
        ]

    def send(step):
        nonlocal last
        sent = send_rows(blocks[step], chosen[step], shape, last)
        last = sent[:1]
        came[step] = [shift(r, dims, seconds[step], d + 1) for d, r in enumerate(sent)]

    def run(step):
        nonlocal last
        results[step] = feed_forward(
            blocks[step], came[step], expert_slices, chosen[step], shape, last
        )
        last = results[step][:1]

    def give(step):
        own_rows, *rest = results[step]
        results[step] = [own_rows] + [
            shift(r, dims, seconds[step], -d - 1) for d, r in enumerate(rest)
        ]

    def join(step, extra=()):
        nonlocal last
        out = combine(blocks[step], results[step], chosen[step], extra, shape, last)
        last = out[:1]
        parts[step] = out[:1] + [
            shift(r, dims, firsts[step], -d - 1) for d, r in enumerate(out[1:])
        ]

    wide = blocks[0]
    if others:
        side = [shift(own[0], dims, "x", d, others) for d in range(1, dims["x"])]
        wide = own[:1] + [
            jnp.where(chosen[0][-1] > 0, b, s) for b, s in zip(blocks[0][1:], side)
        ]
    peers = [shift(b, dims, "c", d) for d in range(1, cores) for b in wide]

    def spread():
        nonlocal last, shared
        shared = feed_forward(
            wide, peers, [[shared_gate.T, shared_up.T, shared_down]], None, shape, last
        )
        last = shared[:1]
        shared = shared[:1] + [shift(r, dims, "c", -d - 1) for d, r in enumerate(shared[1:])]
        for d in range(1, dims["x"] if others else 1):
            span = slice(d * tok_rows, (d + 1) * tok_rows)
            away = sum(r[span].astype(F32) for r in shared).astype(BF16)
            aside.append(shift(away, dims, "x", -d, others))

    shared, aside = [], []
    later = list(range(1, steps))
    loaded = load([w for weights in expert_slices for w in weights], last)
    expert_slices = [loaded[i : i + 3] for i in range(0, len(loaded), 3)]
    last = loaded[-1:]
    for step in [0] + later[:1]:
        send(step)
    for step in [0] + later[:1]:
        run(step)
        give(step)
    for step in later[1:2]:
        send(step)
    spread()
    for step in later[:1]:
        join(step)
    for step in later[1:2]:
        run(step)
        give(step)
    for step in later[2:]:
        send(step)
    join(0, shared)
    for step in later[1:2]:
        join(step)
    for step in later[2:]:
        run(step)
        give(step)
        join(step)

    passed = []
    for step in later + [0]:
        total = parts[step][0]
        for part in parts[step][1:] + passed + ([] if step else aside):
            total = total + part.astype(F32)
        total = total.astype(BF16)
        if step:
            passed = [shift(total, dims, "z", 1)]
    return total


def solution(mesh):
    in_specs = (
        P(AXES, None),
        P(),
        P(),
        P(),
        P(AXES, None),
        P(None, AXES),
        P(None, AXES),
        P(AXES, None),
        P(None, "local"),
        P(None, "local"),
        P("local", None),
    )
    out_specs = P(AXES, None)

    return jax.shard_map(body, mesh=mesh, in_specs=in_specs, out_specs=out_specs, check_vma=False)
```

```python
import math

import jax
import jax.numpy as jnp
import numpy as np
from jax import lax
from jax.experimental import pallas as pl
from jax.experimental.pallas import tpu as pltpu
from jax.sharding import PartitionSpec as P


AXES = ("node", "local")
F32 = jnp.float32
BF16 = jnp.bfloat16
STRIP = 8
UNUSED = -4096.0
PIECE = 256
LIMIT = 10 << 20


def places(dims):
    return [dict(zip(dims, p)) for p in np.ndindex(*dims.values())]


def index_of(dims, place):
    index = 0
    for name, size in dims.items():
        index = index * size + place[name] % size
    return index


def moved(dims, place, axes, step):
    axis = axes[place["c"] % len(axes)]
    return index_of(dims, {**place, axis: place[axis] + step})


def shift(block, dims, axes, step, only=None):
    route = [
        (i, moved(dims, p, axes, step))
        for i, p in enumerate(places(dims))
        if only is None or p["c"] in only
    ]
    return lax.ppermute(block, AXES, route)


def targets(dims, axes, direct):
    size = dims[axes[0]]
    table = [
        [moved(dims, p, axes, d) // dims["c"] for d in range(size)] + [int(p["c"] in direct)]
        for p in places(dims)
    ]
    return lax.dynamic_index_in_dim(
        jnp.asarray(np.array(table, np.int32)), lax.axis_index(AXES), 0, keepdims=False
    )


def routing_rows(normed, router_weight, placement, expert_ids):
    slots = placement.shape[0]
    tok_rows = normed.shape[0]
    slot_iota = jnp.arange(slots, dtype=jnp.int32)
    to_slot = (placement[:, None] == slot_iota).astype(BF16)
    slot_router = jnp.dot(router_weight, to_slot, preferred_element_type=F32).astype(BF16)
    logits = lax.dot_general(slot_router, normed, (((0,), (1,)), ((), ())), preferred_element_type=F32)
    named = expert_ids[:, :, None] == slot_iota
    token_slots = jnp.sum(jnp.where(named, placement, 0), -1)
    hot = jnp.any(token_slots.T[:, None, :] == slot_iota[:, None], 0)
    picked = jnp.where(hot, jax.nn.sigmoid(logits), 0.0)
    gates = picked / jnp.sum(picked, 0, keepdims=True)
    upper = jnp.arange(tok_rows)[:, None] <= jnp.arange(tok_rows)
    running = jnp.dot(hot.astype(BF16), upper.astype(BF16), preferred_element_type=F32)
    return jnp.concatenate([gates, jnp.where(hot, running, UNUSED)], 0).astype(BF16)


def pack(rows, width):
    count, lanes = rows.shape
    strips = -(-count // STRIP)
    rows = jnp.pad(rows, ((0, strips * STRIP - count), (0, 0)))
    parts = [rows[i * STRIP : (i + 1) * STRIP] for i in range(strips)]
    packed = jnp.concatenate(parts, 1)
    return jnp.pad(packed, ((0, 0), (0, width - strips * lanes)))


def table_row(block, tok_rows, row):
    start = pl.multiple_of(row // STRIP * tok_rows, tok_rows)
    group = block[tok_rows : tok_rows + STRIP, pl.ds(start, tok_rows)].astype(F32)
    lines = lax.broadcasted_iota(jnp.int32, group.shape, 0)
    return jnp.sum(jnp.where(lines == row % STRIP, group, 0.0), 0, keepdims=True)


def choice(blocks, tok_rows, slots, slot, list_rows, capacity, gated):
    lines = lax.broadcasted_iota(jnp.int32, (list_rows, tok_rows), 0).astype(F32)
    columns = []
    for i, block in enumerate(blocks):
        place = table_row(block, tok_rows, slots + slot)
        value = table_row(block, tok_rows, slot) if gated else 1.0
        columns.append(jnp.where(lines + float(1 - i * capacity) == place, value, 0.0))
    return jnp.concatenate(columns, 1).astype(BF16)


def stacked(blocks, tok_rows):
    return jnp.concatenate([b[:tok_rows] for b in blocks], 0)


def vmem():
    return pl.BlockSpec(memory_space=pltpu.VMEM)


def kept(arrays, space=pltpu.VMEM):
    return [pltpu.with_memory_space_constraint(a, space) for a in arrays]


def load(arrays, after):
    def kernel(*refs):
        sources, outs, sems = refs[: len(arrays)], refs[-len(arrays) - 1 : -1], refs[-1]
        copies = [pltpu.make_async_copy(s, o, sems.at[i]) for i, (s, o) in enumerate(zip(sources, outs))]
        for copy in copies:
            copy.start()
        for copy in copies:
            copy.wait()

    call = pl.pallas_call(
        kernel,
        out_shape=[pltpu.VMEM(a.shape, a.dtype) for a in arrays],
        in_specs=[anywhere()] * (len(arrays) + len(after)),
        out_specs=[vmem()] * len(arrays),
        scratch_shapes=[pltpu.SemaphoreType.DMA((len(arrays),))],
        compiler_params=pltpu.CompilerParams(vmem_limit_bytes=LIMIT),
        cost_estimate=pl.CostEstimate(flops=1 << 32, bytes_accessed=0, transcendentals=0),
        name="load",
    )
    return list(call(*kept(arrays, pltpu.HBM), *after))


def anywhere():
    return pl.BlockSpec(memory_space=pl.ANY)


def send_rows(blocks, chosen, shape, after):
    slots, tok_rows, capacity, list_rows = shape
    width = blocks[0].shape[1]
    outs = chosen.shape[0] - 2

    def kernel(slot_ref, *refs):
        block_refs = refs[: len(blocks)]
        out_refs = refs[len(refs) - outs :]
        tokens = stacked(block_refs, tok_rows)
        for d, out in enumerate(out_refs):
            hot = choice(block_refs, tok_rows, slots, slot_ref[d + 1], list_rows, capacity, False)
            out[...] = jnp.dot(hot, tokens, preferred_element_type=F32).astype(BF16)

    flops = 2 * outs * list_rows * len(blocks) * tok_rows * width
    call = pl.pallas_call(
        kernel,
        out_shape=[pltpu.VMEM((list_rows, width), BF16)] * outs,
        in_specs=[pl.BlockSpec(memory_space=pltpu.SMEM)]
        + [vmem()] * len(blocks)
        + [anywhere()] * len(after),
        out_specs=[vmem()] * outs,
        cost_estimate=pl.CostEstimate(flops=4 * flops, bytes_accessed=0, transcendentals=0),
        compiler_params=pltpu.CompilerParams(vmem_limit_bytes=LIMIT),
        name="send_rows",
    )
    return list(call(chosen, *kept(blocks), *after))


def feed_forward(blocks, came, slices, chosen, shape, after):
    slots, tok_rows, capacity, list_rows = shape
    width = blocks[0].shape[1]
    routed = chosen is not None
    group = list_rows if routed else len(blocks) * tok_rows
    groups = 1 + (len(came) if routed else len(came) // len(blocks))
    count = group * groups
    hidden = slices[0][0].shape[0]
    pieces = [(lo, min(PIECE, hidden - lo)) for lo in range(0, hidden, PIECE)]

    def kernel(*refs):
        refs = list(refs)
        slot_ref = refs.pop(0) if routed else None
        block_refs = [refs.pop(0) for _ in blocks]
        came_refs = [refs.pop(0) for _ in came]
        weights = [[refs.pop(0) for _ in range(3)] for _ in slices]
        for _ in after:
            refs.pop(0)
        out_refs = [refs.pop(0) for _ in range(groups)]
        rows, active, total, *streamed = refs
        if not routed:
            *stores, sems = streamed

            def copy(i, n, j, part):
                source, store = weights[i][n].at[part], stores[n].at[i, part]
                return pltpu.make_async_copy(source, store, sems.at[i, n, j])

            parts = [pl.ds(lo, size) for lo, size in pieces]
            for i in range(len(slices)):
                for j, part in enumerate(parts):
                    copy(i, 0, j, part).start()
                    copy(i, 1, j, part).start()
                copy(i, 2, 0, pl.ds(0, hidden)).start()

        tokens = stacked(block_refs, tok_rows)
        if routed:
            hot = choice(block_refs, tok_rows, slots, slot_ref[0], list_rows, capacity, False)
            rows[:group] = jnp.dot(hot, tokens, preferred_element_type=F32).astype(BF16)
        else:
            rows[:group] = tokens
        if routed:
            for d, ref in enumerate(came_refs):
                rows[(d + 1) * group : (d + 2) * group] = ref[...]
        else:
            for d, ref in enumerate(came_refs):
                start = group + d * tok_rows
                rows[start : start + tok_rows] = ref[:tok_rows]
        across = (((1,), (1,)), ((), ()))
        for i, (gate_ref, up_ref, down_ref) in enumerate(weights):
            values = rows[...]
            if not routed:
                gate_ref, up_ref, down_ref = [store.at[i] for store in stores]
            for j, (lo, size) in enumerate(pieces):
                span = slice(lo, lo + size)
                if not routed:
                    copy(i, 0, j, parts[j]).wait()
                    copy(i, 1, j, parts[j]).wait()
                gate = lax.dot_general(values, gate_ref[span], across, preferred_element_type=F32)
                up = lax.dot_general(values, up_ref[span], across, preferred_element_type=F32)
                active[:, span] = (gate / (1.0 + jnp.exp(-gate)) * up).astype(BF16)
            if not routed:
                copy(i, 2, 0, pl.ds(0, hidden)).wait()
            part = jnp.dot(active[...], down_ref[...], preferred_element_type=F32)
            if i:
                part = total[...] + part
            if i + 1 < len(weights):
                total[...] = part
                continue
            for d, out in enumerate(out_refs):
                out[...] = part[d * group : (d + 1) * group].astype(out.dtype)

    flops = 6 * count * width * hidden * len(slices)
    operands = [chosen] if routed else []
    stream = []
    if not routed:
        stream = [pltpu.VMEM((len(slices), hidden, width), BF16)] * 3
        stream += [pltpu.SemaphoreType.DMA((len(slices), 3, len(pieces)))]
    call = pl.pallas_call(
        kernel,
        out_shape=[
            pltpu.VMEM((group, width), BF16 if routed or d else F32) for d in range(groups)
        ],
        in_specs=[pl.BlockSpec(memory_space=pltpu.SMEM)] * len(operands)
        + [vmem()] * (len(blocks) + len(came))
        + [vmem() if routed else anywhere()] * (3 * len(slices))
        + [anywhere()] * len(after),
        out_specs=[vmem()] * groups,
        scratch_shapes=[
            pltpu.VMEM((count, width), BF16),
            pltpu.VMEM((count, hidden), BF16),
            pltpu.VMEM((count, width), F32),
        ]
        + stream,
        compiler_params=pltpu.CompilerParams(vmem_limit_bytes=LIMIT if routed else 2 * LIMIT),
        cost_estimate=pl.CostEstimate(flops=flops, bytes_accessed=0, transcendentals=0),
        name="experts" if routed else "shared",
    )
    weights = [w for s in slices for w in s]
    weights = kept(weights, pltpu.VMEM if routed else pltpu.HBM)
    return list(call(*operands, *kept(blocks), *kept(came), *weights, *after))


def combine(blocks, back, chosen, extra, shape, after):
    slots, tok_rows, capacity, list_rows = shape
    width = blocks[0].shape[1]

    def kernel(slot_ref, *refs):
        refs = list(refs)
        block_refs = [refs.pop(0) for _ in blocks]
        back_refs = [refs.pop(0) for _ in back]
        extra_refs = [refs.pop(0) for _ in extra]
        for _ in after:
            refs.pop(0)
        out_refs = refs
        weights = [
            choice(block_refs, tok_rows, slots, slot_ref[d], list_rows, capacity, True)
            for d in range(len(back))
        ]
        for i, out in enumerate(out_refs):
            span = slice(i * tok_rows, (i + 1) * tok_rows)
            sums = None
            for w, ref in zip(weights, back_refs):
                part = lax.dot_general(
                    w[:, span], ref[...], (((0,), (0,)), ((), ())), preferred_element_type=F32
                )
                sums = part if sums is None else sums + part
            for ref in extra_refs:
                more = ref[span].astype(F32)
                sums = sums + (more * slot_ref[len(back)].astype(F32) if i else more)
            out[...] = sums.astype(out.dtype)

    flops = 2 * len(back) * list_rows * len(blocks) * tok_rows * width
    call = pl.pallas_call(
        kernel,
        out_shape=[
            pltpu.VMEM((tok_rows, width), BF16 if i else F32) for i in range(len(blocks))
        ],
        in_specs=[pl.BlockSpec(memory_space=pltpu.SMEM)]
        + [vmem()] * (len(blocks) + len(back) + len(extra))
        + [anywhere()] * len(after),
        out_specs=[vmem()] * len(blocks),
        cost_estimate=pl.CostEstimate(flops=4 * flops, bytes_accessed=0, transcendentals=0),
        compiler_params=pltpu.CompilerParams(vmem_limit_bytes=LIMIT),
        name="combine",
    )
    return list(call(chosen, *kept(blocks), *kept(back), *kept(extra), *after))


def body(
    tokens,
    norm_gain,
    router_weight,
    placement,
    expert_ids,
    w_gate,
    w_up,
    w_down,
    shared_gate,
    shared_up,
    shared_down,
):
    slots = placement.shape[0]
    tok_rows, width = tokens.shape
    capacity = 3 * tok_rows * expert_ids.shape[1] // (2 * slots)
    node_count = lax.axis_size("node")
    local_count = lax.axis_size("local")
    cores = node_count * local_count // slots
    x_count = local_count // cores
    y_count = math.gcd(node_count, x_count)
    dims = {"z": node_count // y_count, "y": y_count, "x": x_count, "c": cores}
    list_rows = -(-x_count * capacity // 16) * 16
    shape = (slots, tok_rows, capacity, list_rows)
    steps = dims["z"]
    mixed = ("xy", "yx") if x_count == y_count else ("xy", "xy")
    orders = [mixed] * steps
    direct = [c for c in range(cores) if mixed[c % 2][0] == "x"]
    others = [c for c in range(cores) if c not in direct]

    def slices_of(*weights):
        return [list(weights)] + [
            [shift(w, dims, "c", step) for w in weights] for step in range(1, cores)
        ]

    expert_slices = slices_of(w_gate.T, w_up.T, w_down)

    floats = tokens.astype(F32)
    normed = (
        floats * lax.rsqrt(jnp.mean(floats * floats, -1, keepdims=True) + 1e-06) * norm_gain
    ).astype(BF16)
    routing = routing_rows(normed, router_weight, placement, expert_ids)
    own = [jnp.concatenate([normed, pack(routing, width)], 0)]
    for _ in range(1, steps):
        own.append(shift(own[-1], dims, "z", 1))

    last = own[:1]
    blocks, chosen, came, results, parts = {}, {}, {}, {}, {}
    firsts = [[o[0] for o in order] for order in orders]
    seconds = [[o[1] for o in order] for order in orders]
    for step in range(steps):
        chosen[step] = targets(dims, seconds[step], direct)
        blocks[step] = [own[step]] + [
            shift(own[step], dims, firsts[step], d) for d in range(1, dims[firsts[step][0]])
        ]

    def send(step):
        nonlocal last
        sent = send_rows(blocks[step], chosen[step], shape, last)
        last = sent[:1]
        came[step] = [shift(r, dims, seconds[step], d + 1) for d, r in enumerate(sent)]

    def run(step):
        nonlocal last
        results[step] = feed_forward(
            blocks[step], came[step], expert_slices, chosen[step], shape, last
        )
        last = results[step][:1]

    def give(step):
        own_rows, *rest = results[step]
        results[step] = [own_rows] + [
            shift(r, dims, seconds[step], -d - 1) for d, r in enumerate(rest)
        ]

    def join(step, extra=()):
        nonlocal last
        out = combine(blocks[step], results[step], chosen[step], extra, shape, last)
        last = out[:1]
        parts[step] = out[:1] + [
            shift(r, dims, firsts[step], -d - 1) for d, r in enumerate(out[1:])
        ]

    wide = blocks[0]
    if others:
        side = [shift(own[0], dims, "x", d, others) for d in range(1, dims["x"])]
        wide = own[:1] + [
            jnp.where(chosen[0][-1] > 0, b, s) for b, s in zip(blocks[0][1:], side)
        ]
    peers = [shift(b, dims, "c", d) for d in range(1, cores) for b in wide]

    def spread():
        nonlocal last, shared
        shared = feed_forward(
            wide, peers, [[shared_gate.T, shared_up.T, shared_down]], None, shape, last
        )
        last = shared[:1]
        shared = shared[:1] + [shift(r, dims, "c", -d - 1) for d, r in enumerate(shared[1:])]
        for d in range(1, dims["x"] if others else 1):
            span = slice(d * tok_rows, (d + 1) * tok_rows)
            away = sum(r[span].astype(F32) for r in shared).astype(BF16)
            aside.append(shift(away, dims, "x", -d, others))

    shared, aside = [], []
    later = list(range(1, steps))

    def fill(number):
        nonlocal last
        expert_slices[number] = load(expert_slices[number], last)
        last = expert_slices[number][-1:]

    fill(0)
    send(0)
    for number in range(1, cores):
        fill(number)
    run(0)
    for step in later[:1]:
        send(step)
    give(0)
    for step in later[:1]:
        run(step)
        give(step)
    for step in later[1:2]:
        send(step)
    for step in later[:1]:
        join(step)
    for step in later[1:2]:
        run(step)
        give(step)
    for step in later[2:]:
        send(step)
    spread()
    for step in later[1:2]:
        join(step)
    for step in later[2:]:
        run(step)
        give(step)
    join(0, shared)
    for step in later[2:]:
        join(step)

    passed = []
    for step in later + [0]:
        total = parts[step][0]
        for part in parts[step][1:] + passed + ([] if step else aside):
            total = total + part.astype(F32)
        total = total.astype(BF16)
        if step:
            passed = [shift(total, dims, "z", 1)]
    return total


def solution(mesh):
    in_specs = (
        P(AXES, None),
        P(),
        P(),
        P(),
        P(AXES, None),
        P(None, AXES),
        P(None, AXES),
        P(AXES, None),
        P(None, "local"),
        P(None, "local"),
        P("local", None),
    )
    out_specs = P(AXES, None)

    return jax.shard_map(body, mesh=mesh, in_specs=in_specs, out_specs=out_specs, check_vma=False)
```

```python
import math

import jax
import jax.numpy as jnp
import numpy as np
from jax import lax
from jax.experimental import pallas as pl
from jax.experimental.pallas import tpu as pltpu
from jax.sharding import PartitionSpec as P


AXES = ("node", "local")
F32 = jnp.float32
BF16 = jnp.bfloat16
STRIP = 8
UNUSED = -4096.0
PIECE = 256
LIMIT = 10 << 20


def places(dims):
    return [dict(zip(dims, p)) for p in np.ndindex(*dims.values())]


def index_of(dims, place):
    index = 0
    for name, size in dims.items():
        index = index * size + place[name] % size
    return index


def moved(dims, place, axes, step):
    axis = axes[place["c"] % len(axes)]
    return index_of(dims, {**place, axis: place[axis] + step})


def shift(block, dims, axes, step):
    route = [(i, moved(dims, p, axes, step)) for i, p in enumerate(places(dims))]
    return lax.ppermute(block, AXES, route)


def targets(dims, axes):
    size = dims[axes[0]]
    table = [[moved(dims, p, axes, d) // dims["c"] for d in range(size)] for p in places(dims)]
    return lax.dynamic_index_in_dim(
        jnp.asarray(np.array(table, np.int32)), lax.axis_index(AXES), 0, keepdims=False
    )


def routing_rows(normed, router_weight, placement, expert_ids):
    slots = placement.shape[0]
    tok_rows = normed.shape[0]
    slot_iota = jnp.arange(slots, dtype=jnp.int32)
    to_slot = (placement[:, None] == slot_iota).astype(BF16)
    slot_router = jnp.dot(router_weight, to_slot, preferred_element_type=F32).astype(BF16)
    logits = lax.dot_general(slot_router, normed, (((0,), (1,)), ((), ())), preferred_element_type=F32)
    named = expert_ids[:, :, None] == slot_iota
    token_slots = jnp.sum(jnp.where(named, placement, 0), -1)
    hot = jnp.any(token_slots.T[:, None, :] == slot_iota[:, None], 0)
    picked = jnp.where(hot, jax.nn.sigmoid(logits), 0.0)
    gates = picked / jnp.sum(picked, 0, keepdims=True)
    upper = jnp.arange(tok_rows)[:, None] <= jnp.arange(tok_rows)
    running = jnp.dot(hot.astype(BF16), upper.astype(BF16), preferred_element_type=F32)
    return jnp.concatenate([gates, jnp.where(hot, running, UNUSED)], 0).astype(BF16)


def pack(rows, width):
    count, lanes = rows.shape
    strips = -(-count // STRIP)
    rows = jnp.pad(rows, ((0, strips * STRIP - count), (0, 0)))
    parts = [rows[i * STRIP : (i + 1) * STRIP] for i in range(strips)]
    packed = jnp.concatenate(parts, 1)
    return jnp.pad(packed, ((0, 0), (0, width - strips * lanes)))


def table_row(block, tok_rows, row):
    start = pl.multiple_of(row // STRIP * tok_rows, tok_rows)
    group = block[tok_rows : tok_rows + STRIP, pl.ds(start, tok_rows)].astype(F32)
    lines = lax.broadcasted_iota(jnp.int32, group.shape, 0)
    return jnp.sum(jnp.where(lines == row % STRIP, group, 0.0), 0, keepdims=True)


def choice(blocks, tok_rows, slots, slot, list_rows, capacity, gated):
    lines = lax.broadcasted_iota(jnp.int32, (list_rows, tok_rows), 0).astype(F32)
    columns = []
    for i, block in enumerate(blocks):
        place = table_row(block, tok_rows, slots + slot)
        value = table_row(block, tok_rows, slot) if gated else 1.0
        columns.append(jnp.where(lines + float(1 - i * capacity) == place, value, 0.0))
    return jnp.concatenate(columns, 1).astype(BF16)


def stacked(blocks, tok_rows):
    return jnp.concatenate([b[:tok_rows] for b in blocks], 0)


def vmem():
    return pl.BlockSpec(memory_space=pltpu.VMEM)


def kept(arrays, space=pltpu.VMEM):
    return [pltpu.with_memory_space_constraint(a, space) for a in arrays]


def load(arrays, after):
    def kernel(*refs):
        sources, outs, sems = refs[: len(arrays)], refs[-len(arrays) - 1 : -1], refs[-1]
        copies = [pltpu.make_async_copy(s, o, sems.at[i]) for i, (s, o) in enumerate(zip(sources, outs))]
        for copy in copies:
            copy.start()
        for copy in copies:
            copy.wait()

    call = pl.pallas_call(
        kernel,
        out_shape=[pltpu.VMEM(a.shape, a.dtype) for a in arrays],
        in_specs=[anywhere()] * (len(arrays) + len(after)),
        out_specs=[vmem()] * len(arrays),
        scratch_shapes=[pltpu.SemaphoreType.DMA((len(arrays),))],
        compiler_params=pltpu.CompilerParams(vmem_limit_bytes=LIMIT),
        cost_estimate=pl.CostEstimate(flops=1 << 32, bytes_accessed=0, transcendentals=0),
        name="load",
    )
    return list(call(*kept(arrays, pltpu.HBM), *after))


def anywhere():
    return pl.BlockSpec(memory_space=pl.ANY)


def send_rows(blocks, chosen, shape, after):
    slots, tok_rows, capacity, list_rows = shape
    width = blocks[0].shape[1]
    outs = chosen.shape[0] - 1

    def kernel(slot_ref, *refs):
        block_refs = refs[: len(blocks)]
        out_refs = refs[len(refs) - outs :]
        tokens = stacked(block_refs, tok_rows)
        for d, out in enumerate(out_refs):
            hot = choice(block_refs, tok_rows, slots, slot_ref[d + 1], list_rows, capacity, False)
            out[...] = jnp.dot(hot, tokens, preferred_element_type=F32).astype(BF16)

    flops = 2 * outs * list_rows * len(blocks) * tok_rows * width
    call = pl.pallas_call(
        kernel,
        out_shape=[pltpu.VMEM((list_rows, width), BF16)] * outs,
        in_specs=[pl.BlockSpec(memory_space=pltpu.SMEM)]
        + [vmem()] * len(blocks)
        + [anywhere()] * len(after),
        out_specs=[vmem()] * outs,
        cost_estimate=pl.CostEstimate(flops=4 * flops, bytes_accessed=0, transcendentals=0),
        compiler_params=pltpu.CompilerParams(vmem_limit_bytes=LIMIT),
        name="send_rows",
    )
    return list(call(chosen, *kept(blocks), *after))


def feed_forward(blocks, came, slices, chosen, shape, after):
    slots, tok_rows, capacity, list_rows = shape
    width = blocks[0].shape[1]
    routed = chosen is not None
    group = list_rows if routed else len(blocks) * tok_rows
    groups = 1 + (len(came) if routed else len(came) // len(blocks))
    count = group * groups
    hidden = slices[0][0].shape[0]
    pieces = [(lo, min(PIECE, hidden - lo)) for lo in range(0, hidden, PIECE)]

    def kernel(*refs):
        refs = list(refs)
        slot_ref = refs.pop(0) if routed else None
        block_refs = [refs.pop(0) for _ in blocks]
        came_refs = [refs.pop(0) for _ in came]
        weights = [[refs.pop(0) for _ in range(3)] for _ in slices]
        for _ in after:
            refs.pop(0)
        out_refs = [refs.pop(0) for _ in range(groups)]
        rows, active, total, *streamed = refs
        if not routed:
            *stores, sems = streamed

            def copy(i, n, j, part):
                source, store = weights[i][n].at[part], stores[n].at[i, part]
                return pltpu.make_async_copy(source, store, sems.at[i, n, j])

            parts = [pl.ds(lo, size) for lo, size in pieces]
            for i in range(len(slices)):
                for j, part in enumerate(parts):
                    copy(i, 0, j, part).start()
                    copy(i, 1, j, part).start()
                copy(i, 2, 0, pl.ds(0, hidden)).start()

        tokens = stacked(block_refs, tok_rows)
        if routed:
            hot = choice(block_refs, tok_rows, slots, slot_ref[0], list_rows, capacity, False)
            rows[:group] = jnp.dot(hot, tokens, preferred_element_type=F32).astype(BF16)
        else:
            rows[:group] = tokens
        if routed:
            for d, ref in enumerate(came_refs):
                rows[(d + 1) * group : (d + 2) * group] = ref[...]
        else:
            for d, ref in enumerate(came_refs):
                start = group + d * tok_rows
                rows[start : start + tok_rows] = ref[:tok_rows]
        across = (((1,), (1,)), ((), ()))
        for i, (gate_ref, up_ref, down_ref) in enumerate(weights):
            values = rows[...]
            if not routed:
                gate_ref, up_ref, down_ref = [store.at[i] for store in stores]
            for j, (lo, size) in enumerate(pieces):
                span = slice(lo, lo + size)
                if not routed:
                    copy(i, 0, j, parts[j]).wait()
                    copy(i, 1, j, parts[j]).wait()
                gate = lax.dot_general(values, gate_ref[span], across, preferred_element_type=F32)
                up = lax.dot_general(values, up_ref[span], across, preferred_element_type=F32)
                active[:, span] = (gate / (1.0 + jnp.exp(-gate)) * up).astype(BF16)
            if not routed:
                copy(i, 2, 0, pl.ds(0, hidden)).wait()
            part = jnp.dot(active[...], down_ref[...], preferred_element_type=F32)
            if i:
                part = total[...] + part
            if i + 1 < len(weights):
                total[...] = part
                continue
            for d, out in enumerate(out_refs):
                out[...] = part[d * group : (d + 1) * group].astype(out.dtype)

    flops = 6 * count * width * hidden * len(slices)
    operands = [chosen] if routed else []
    stream = []
    if not routed:
        stream = [pltpu.VMEM((len(slices), hidden, width), BF16)] * 3
        stream += [pltpu.SemaphoreType.DMA((len(slices), 3, len(pieces)))]
    call = pl.pallas_call(
        kernel,
        out_shape=[
            pltpu.VMEM((group, width), BF16 if routed or d else F32) for d in range(groups)
        ],
        in_specs=[pl.BlockSpec(memory_space=pltpu.SMEM)] * len(operands)
        + [vmem()] * (len(blocks) + len(came))
        + [vmem() if routed else anywhere()] * (3 * len(slices))
        + [anywhere()] * len(after),
        out_specs=[vmem()] * groups,
        scratch_shapes=[
            pltpu.VMEM((count, width), BF16),
            pltpu.VMEM((count, hidden), BF16),
            pltpu.VMEM((count, width), F32),
        ]
        + stream,
        compiler_params=pltpu.CompilerParams(vmem_limit_bytes=LIMIT if routed else 2 * LIMIT),
        cost_estimate=pl.CostEstimate(flops=flops, bytes_accessed=0, transcendentals=0),
        name="experts" if routed else "shared",
    )
    weights = [w for s in slices for w in s]
    weights = kept(weights, pltpu.VMEM if routed else pltpu.HBM)
    return list(call(*operands, *kept(blocks), *kept(came), *weights, *after))


def combine(blocks, back, chosen, extra, shape, after):
    slots, tok_rows, capacity, list_rows = shape
    width = blocks[0].shape[1]

    def kernel(slot_ref, *refs):
        refs = list(refs)
        block_refs = [refs.pop(0) for _ in blocks]
        back_refs = [refs.pop(0) for _ in back]
        extra_refs = [refs.pop(0) for _ in extra]
        for _ in after:
            refs.pop(0)
        out_refs = refs
        weights = [
            choice(block_refs, tok_rows, slots, slot_ref[d], list_rows, capacity, True)
            for d in range(len(back))
        ]
        for i, out in enumerate(out_refs):
            span = slice(i * tok_rows, (i + 1) * tok_rows)
            sums = None
            for w, ref in zip(weights, back_refs):
                part = lax.dot_general(
                    w[:, span], ref[...], (((0,), (0,)), ((), ())), preferred_element_type=F32
                )
                sums = part if sums is None else sums + part
            for ref in extra_refs:
                sums = sums + ref[span]
            out[...] = sums.astype(out.dtype)

    flops = 2 * len(back) * list_rows * len(blocks) * tok_rows * width
    call = pl.pallas_call(
        kernel,
        out_shape=[
            pltpu.VMEM((tok_rows, width), BF16 if i else F32) for i in range(len(blocks))
        ],
        in_specs=[pl.BlockSpec(memory_space=pltpu.SMEM)]
        + [vmem()] * (len(blocks) + len(back) + len(extra))
        + [anywhere()] * len(after),
        out_specs=[vmem()] * len(blocks),
        cost_estimate=pl.CostEstimate(flops=4 * flops, bytes_accessed=0, transcendentals=0),
        compiler_params=pltpu.CompilerParams(vmem_limit_bytes=LIMIT),
        name="combine",
    )
    return list(call(chosen, *kept(blocks), *kept(back), *kept(extra), *after))


def body(
    tokens,
    norm_gain,
    router_weight,
    placement,
    expert_ids,
    w_gate,
    w_up,
    w_down,
    shared_gate,
    shared_up,
    shared_down,
):
    slots = placement.shape[0]
    tok_rows, width = tokens.shape
    capacity = 3 * tok_rows * expert_ids.shape[1] // (2 * slots)
    node_count = lax.axis_size("node")
    local_count = lax.axis_size("local")
    cores = node_count * local_count // slots
    x_count = local_count // cores
    y_count = math.gcd(node_count, x_count)
    dims = {"z": node_count // y_count, "y": y_count, "x": x_count, "c": cores}
    list_rows = -(-x_count * capacity // 16) * 16
    shape = (slots, tok_rows, capacity, list_rows)
    steps = dims["z"]
    mixed = ("xy", "yx") if x_count == y_count else ("xy", "xy")
    orders = [("xy", "xy")] + [mixed] * (steps - 1)

    def slices_of(*weights):
        return [list(weights)] + [
            [shift(w, dims, "c", step) for w in weights] for step in range(1, cores)
        ]

    expert_slices = slices_of(w_gate.T, w_up.T, w_down)

    floats = tokens.astype(F32)
    normed = (
        floats * lax.rsqrt(jnp.mean(floats * floats, -1, keepdims=True) + 1e-06) * norm_gain
    ).astype(BF16)
    routing = routing_rows(normed, router_weight, placement, expert_ids)
    own = [jnp.concatenate([normed, pack(routing, width)], 0)]
    for _ in range(1, steps):
        own.append(shift(own[-1], dims, "z", 1))

    last = own[:1]
    blocks, chosen, came, results, parts = {}, {}, {}, {}, {}
    firsts = [[o[0] for o in order] for order in orders]
    seconds = [[o[1] for o in order] for order in orders]
    for step in range(steps):
        chosen[step] = targets(dims, seconds[step])
        blocks[step] = [own[step]] + [
            shift(own[step], dims, firsts[step], d) for d in range(1, dims[firsts[step][0]])
        ]

    def send(step):
        nonlocal last
        sent = send_rows(blocks[step], chosen[step], shape, last)
        last = sent[:1]
        came[step] = [shift(r, dims, seconds[step], d + 1) for d, r in enumerate(sent)]

    def run(step):
        nonlocal last
        results[step] = feed_forward(
            blocks[step], came[step], expert_slices, chosen[step], shape, last
        )
        last = results[step][:1]

    def give(step):
        own_rows, *rest = results[step]
        results[step] = [own_rows] + [
            shift(r, dims, seconds[step], -d - 1) for d, r in enumerate(rest)
        ]

    def join(step, extra=()):
        nonlocal last
        out = combine(blocks[step], results[step], chosen[step], extra, shape, last)
        last = out[:1]
        parts[step] = out[:1] + [
            shift(r, dims, firsts[step], -d - 1) for d, r in enumerate(out[1:])
        ]

    def spread():
        nonlocal last, shared
        peers = [shift(b, dims, "c", d) for d in range(1, cores) for b in blocks[0]]
        shared = feed_forward(
            blocks[0], peers, [[shared_gate.T, shared_up.T, shared_down]], None, shape, last
        )
        last = shared[:1]
        shared = shared[:1] + [shift(r, dims, "c", -d - 1) for d, r in enumerate(shared[1:])]

    shared = []
    later = list(range(1, steps))
    for step in [0] + later[:1]:
        send(step)
    loaded = load([w for weights in expert_slices for w in weights], last)
    expert_slices = [loaded[i : i + 3] for i in range(0, len(loaded), 3)]
    last = loaded[-1:]
    spread()
    for step in later[1:2]:
        send(step)
    for step in later[:1] + [0]:
        run(step)
    for step in later[:1]:
        give(step)
    for step in later[2:]:
        send(step)
    for step in later[:1]:
        join(step)
    for step in later[1:]:
        run(step)
        give(step)
    give(0)
    for step in later[1:]:
        join(step)
    join(0, shared)

    passed = []
    for step in later + [0]:
        total = parts[step][0]
        for part in parts[step][1:] + passed:
            total = total + part.astype(F32)
        total = total.astype(BF16)
        if step:
            passed = [shift(total, dims, "z", 1)]
    return total


def solution(mesh):
    in_specs = (
        P(AXES, None),
        P(),
        P(),
        P(),
        P(AXES, None),
        P(None, AXES),
        P(None, AXES),
        P(AXES, None),
        P(None, "local"),
        P(None, "local"),
        P("local", None),
    )
    out_specs = P(AXES, None)

    return jax.shard_map(body, mesh=mesh, in_specs=in_specs, out_specs=out_specs, check_vma=False)
```

```python
import math

import jax
import jax.numpy as jnp
import numpy as np
from jax import lax
from jax.experimental import pallas as pl
from jax.experimental.pallas import tpu as pltpu
from jax.sharding import PartitionSpec as P


AXES = ("node", "local")
F32 = jnp.float32
BF16 = jnp.bfloat16
STRIP = 8
UNUSED = -4096.0
PIECE = 256
LIMIT = 10 << 20


def places(dims):
    return [dict(zip(dims, p)) for p in np.ndindex(*dims.values())]


def index_of(dims, place):
    index = 0
    for name, size in dims.items():
        index = index * size + place[name] % size
    return index


def moved(dims, place, axes, step):
    axis = axes[place["c"] % len(axes)]
    return index_of(dims, {**place, axis: place[axis] + step})


def shift(block, dims, axes, step):
    route = [(i, moved(dims, p, axes, step)) for i, p in enumerate(places(dims))]
    return lax.ppermute(block, AXES, route)


def targets(dims, axes):
    size = dims[axes[0]]
    table = [[moved(dims, p, axes, d) // dims["c"] for d in range(size)] for p in places(dims)]
    return lax.dynamic_index_in_dim(
        jnp.asarray(np.array(table, np.int32)), lax.axis_index(AXES), 0, keepdims=False
    )


def routing_rows(normed, router_weight, placement, expert_ids):
    slots = placement.shape[0]
    tok_rows = normed.shape[0]
    slot_iota = jnp.arange(slots, dtype=jnp.int32)
    to_slot = (placement[:, None] == slot_iota).astype(BF16)
    slot_router = jnp.dot(router_weight, to_slot, preferred_element_type=F32).astype(BF16)
    logits = lax.dot_general(slot_router, normed, (((0,), (1,)), ((), ())), preferred_element_type=F32)
    named = expert_ids[:, :, None] == slot_iota
    token_slots = jnp.sum(jnp.where(named, placement, 0), -1)
    hot = jnp.any(token_slots.T[:, None, :] == slot_iota[:, None], 0)
    picked = jnp.where(hot, jax.nn.sigmoid(logits), 0.0)
    gates = picked / jnp.sum(picked, 0, keepdims=True)
    upper = jnp.arange(tok_rows)[:, None] <= jnp.arange(tok_rows)
    running = jnp.dot(hot.astype(BF16), upper.astype(BF16), preferred_element_type=F32)
    return jnp.concatenate([gates, jnp.where(hot, running, UNUSED)], 0).astype(BF16)


def pack(rows, width):
    count, lanes = rows.shape
    strips = -(-count // STRIP)
    rows = jnp.pad(rows, ((0, strips * STRIP - count), (0, 0)))
    parts = [rows[i * STRIP : (i + 1) * STRIP] for i in range(strips)]
    packed = jnp.concatenate(parts, 1)
    return jnp.pad(packed, ((0, 0), (0, width - strips * lanes)))


def table_row(block, tok_rows, row):
    start = pl.multiple_of(row // STRIP * tok_rows, tok_rows)
    group = block[tok_rows : tok_rows + STRIP, pl.ds(start, tok_rows)].astype(F32)
    lines = lax.broadcasted_iota(jnp.int32, group.shape, 0)
    return jnp.sum(jnp.where(lines == row % STRIP, group, 0.0), 0, keepdims=True)


def choice(blocks, tok_rows, slots, slot, list_rows, capacity, gated):
    lines = lax.broadcasted_iota(jnp.int32, (list_rows, tok_rows), 0).astype(F32)
    columns = []
    for i, block in enumerate(blocks):
        place = table_row(block, tok_rows, slots + slot)
        value = table_row(block, tok_rows, slot) if gated else 1.0
        columns.append(jnp.where(lines + float(1 - i * capacity) == place, value, 0.0))
    return jnp.concatenate(columns, 1).astype(BF16)


def stacked(blocks, tok_rows):
    return jnp.concatenate([b[:tok_rows] for b in blocks], 0)


def vmem():
    return pl.BlockSpec(memory_space=pltpu.VMEM)


def kept(arrays, space=pltpu.VMEM):
    return [pltpu.with_memory_space_constraint(a, space) for a in arrays]


def load(arrays, after):
    def kernel(*refs):
        sources, outs, sems = refs[: len(arrays)], refs[-len(arrays) - 1 : -1], refs[-1]
        copies = [pltpu.make_async_copy(s, o, sems.at[i]) for i, (s, o) in enumerate(zip(sources, outs))]
        for copy in copies:
            copy.start()
        for copy in copies:
            copy.wait()

    call = pl.pallas_call(
        kernel,
        out_shape=[pltpu.VMEM(a.shape, a.dtype) for a in arrays],
        in_specs=[anywhere()] * (len(arrays) + len(after)),
        out_specs=[vmem()] * len(arrays),
        scratch_shapes=[pltpu.SemaphoreType.DMA((len(arrays),))],
        compiler_params=pltpu.CompilerParams(vmem_limit_bytes=LIMIT),
        cost_estimate=pl.CostEstimate(flops=1 << 32, bytes_accessed=0, transcendentals=0),
        name="load",
    )
    return list(call(*kept(arrays, pltpu.HBM), *after))


def anywhere():
    return pl.BlockSpec(memory_space=pl.ANY)


def send_rows(blocks, chosen, shape, after):
    slots, tok_rows, capacity, list_rows = shape
    width = blocks[0].shape[1]
    outs = chosen.shape[0] - 1

    def kernel(slot_ref, *refs):
        block_refs = refs[: len(blocks)]
        out_refs = refs[len(refs) - outs :]
        tokens = stacked(block_refs, tok_rows)
        for d, out in enumerate(out_refs):
            hot = choice(block_refs, tok_rows, slots, slot_ref[d + 1], list_rows, capacity, False)
            out[...] = jnp.dot(hot, tokens, preferred_element_type=F32).astype(BF16)

    flops = 2 * outs * list_rows * len(blocks) * tok_rows * width
    call = pl.pallas_call(
        kernel,
        out_shape=[pltpu.VMEM((list_rows, width), BF16)] * outs,
        in_specs=[pl.BlockSpec(memory_space=pltpu.SMEM)]
        + [vmem()] * len(blocks)
        + [anywhere()] * len(after),
        out_specs=[vmem()] * outs,
        cost_estimate=pl.CostEstimate(flops=4 * flops, bytes_accessed=0, transcendentals=0),
        compiler_params=pltpu.CompilerParams(vmem_limit_bytes=LIMIT),
        name="send_rows",
    )
    return list(call(chosen, *kept(blocks), *after))


def feed_forward(blocks, came, slices, chosen, shape, after):
    slots, tok_rows, capacity, list_rows = shape
    width = blocks[0].shape[1]
    routed = chosen is not None
    group = list_rows if routed else len(blocks) * tok_rows
    groups = 1 + (len(came) if routed else len(came) // len(blocks))
    count = group * groups
    hidden = slices[0][0].shape[0]
    pieces = [(lo, min(PIECE, hidden - lo)) for lo in range(0, hidden, PIECE)]

    def kernel(*refs):
        refs = list(refs)
        slot_ref = refs.pop(0) if routed else None
        block_refs = [refs.pop(0) for _ in blocks]
        came_refs = [refs.pop(0) for _ in came]
        weights = [[refs.pop(0) for _ in range(3)] for _ in slices]
        for _ in after:
            refs.pop(0)
        out_refs = [refs.pop(0) for _ in range(groups)]
        rows, active, total, *streamed = refs
        if not routed:
            *stores, sems = streamed

            def copy(i, n, j, part):
                source, store = weights[i][n].at[part], stores[n].at[i, part]
                return pltpu.make_async_copy(source, store, sems.at[i, n, j])

            parts = [pl.ds(lo, size) for lo, size in pieces]
            for i in range(len(slices)):
                for j, part in enumerate(parts):
                    copy(i, 0, j, part).start()
                    copy(i, 1, j, part).start()
                copy(i, 2, 0, pl.ds(0, hidden)).start()

        tokens = stacked(block_refs, tok_rows)
        if routed:
            hot = choice(block_refs, tok_rows, slots, slot_ref[0], list_rows, capacity, False)
            rows[:group] = jnp.dot(hot, tokens, preferred_element_type=F32).astype(BF16)
        else:
            rows[:group] = tokens
        if routed:
            for d, ref in enumerate(came_refs):
                rows[(d + 1) * group : (d + 2) * group] = ref[...]
        else:
            for d, ref in enumerate(came_refs):
                start = group + d * tok_rows
                rows[start : start + tok_rows] = ref[:tok_rows]
        across = (((1,), (1,)), ((), ()))
        for i, (gate_ref, up_ref, down_ref) in enumerate(weights):
            values = rows[...]
            if not routed:
                gate_ref, up_ref, down_ref = [store.at[i] for store in stores]
            for j, (lo, size) in enumerate(pieces):
                span = slice(lo, lo + size)
                if not routed:
                    copy(i, 0, j, parts[j]).wait()
                    copy(i, 1, j, parts[j]).wait()
                gate = lax.dot_general(values, gate_ref[span], across, preferred_element_type=F32)
                up = lax.dot_general(values, up_ref[span], across, preferred_element_type=F32)
                active[:, span] = (gate / (1.0 + jnp.exp(-gate)) * up).astype(BF16)
            if not routed:
                copy(i, 2, 0, pl.ds(0, hidden)).wait()
            part = jnp.dot(active[...], down_ref[...], preferred_element_type=F32)
            if i:
                part = total[...] + part
            if i + 1 < len(weights):
                total[...] = part
                continue
            for d, out in enumerate(out_refs):
                out[...] = part[d * group : (d + 1) * group].astype(out.dtype)

    flops = 6 * count * width * hidden * len(slices)
    operands = [chosen] if routed else []
    stream = []
    if not routed:
        stream = [pltpu.VMEM((len(slices), hidden, width), BF16)] * 3
        stream += [pltpu.SemaphoreType.DMA((len(slices), 3, len(pieces)))]
    call = pl.pallas_call(
        kernel,
        out_shape=[
            pltpu.VMEM((group, width), BF16 if routed or d else F32) for d in range(groups)
        ],
        in_specs=[pl.BlockSpec(memory_space=pltpu.SMEM)] * len(operands)
        + [vmem()] * (len(blocks) + len(came))
        + [vmem() if routed else anywhere()] * (3 * len(slices))
        + [anywhere()] * len(after),
        out_specs=[vmem()] * groups,
        scratch_shapes=[
            pltpu.VMEM((count, width), BF16),
            pltpu.VMEM((count, hidden), BF16),
            pltpu.VMEM((count, width), F32),
        ]
        + stream,
        compiler_params=pltpu.CompilerParams(vmem_limit_bytes=LIMIT if routed else 2 * LIMIT),
        cost_estimate=pl.CostEstimate(flops=flops, bytes_accessed=0, transcendentals=0),
        name="experts" if routed else "shared",
    )
    weights = [w for s in slices for w in s]
    weights = kept(weights, pltpu.VMEM if routed else pltpu.HBM)
    return list(call(*operands, *kept(blocks), *kept(came), *weights, *after))


def combine(blocks, back, chosen, extra, shape, after):
    slots, tok_rows, capacity, list_rows = shape
    width = blocks[0].shape[1]

    def kernel(slot_ref, *refs):
        refs = list(refs)
        block_refs = [refs.pop(0) for _ in blocks]
        back_refs = [refs.pop(0) for _ in back]
        extra_refs = [refs.pop(0) for _ in extra]
        for _ in after:
            refs.pop(0)
        out_refs = refs
        weights = [
            choice(block_refs, tok_rows, slots, slot_ref[d], list_rows, capacity, True)
            for d in range(len(back))
        ]
        for i, out in enumerate(out_refs):
            span = slice(i * tok_rows, (i + 1) * tok_rows)
            sums = None
            for w, ref in zip(weights, back_refs):
                part = lax.dot_general(
                    w[:, span], ref[...], (((0,), (0,)), ((), ())), preferred_element_type=F32
                )
                sums = part if sums is None else sums + part
            for ref in extra_refs:
                sums = sums + ref[span]
            out[...] = sums.astype(out.dtype)

    flops = 2 * len(back) * list_rows * len(blocks) * tok_rows * width
    call = pl.pallas_call(
        kernel,
        out_shape=[
            pltpu.VMEM((tok_rows, width), BF16 if i else F32) for i in range(len(blocks))
        ],
        in_specs=[pl.BlockSpec(memory_space=pltpu.SMEM)]
        + [vmem()] * (len(blocks) + len(back) + len(extra))
        + [anywhere()] * len(after),
        out_specs=[vmem()] * len(blocks),
        cost_estimate=pl.CostEstimate(flops=4 * flops, bytes_accessed=0, transcendentals=0),
        compiler_params=pltpu.CompilerParams(vmem_limit_bytes=LIMIT),
        name="combine",
    )
    return list(call(chosen, *kept(blocks), *kept(back), *kept(extra), *after))


def body(
    tokens,
    norm_gain,
    router_weight,
    placement,
    expert_ids,
    w_gate,
    w_up,
    w_down,
    shared_gate,
    shared_up,
    shared_down,
):
    slots = placement.shape[0]
    tok_rows, width = tokens.shape
    capacity = 3 * tok_rows * expert_ids.shape[1] // (2 * slots)
    node_count = lax.axis_size("node")
    local_count = lax.axis_size("local")
    cores = node_count * local_count // slots
    x_count = local_count // cores
    y_count = math.gcd(node_count, x_count)
    dims = {"z": node_count // y_count, "y": y_count, "x": x_count, "c": cores}
    list_rows = -(-x_count * capacity // 16) * 16
    shape = (slots, tok_rows, capacity, list_rows)
    steps = dims["z"]
    mixed = ("xy", "yx") if x_count == y_count else ("xy", "xy")
    orders = [("xy", "xy")] + [mixed] * (steps - 1)

    def slices_of(*weights):
        return [list(weights)] + [
            [shift(w, dims, "c", step) for w in weights] for step in range(1, cores)
        ]

    expert_slices = slices_of(w_gate.T, w_up.T, w_down)

    floats = tokens.astype(F32)
    normed = (
        floats * lax.rsqrt(jnp.mean(floats * floats, -1, keepdims=True) + 1e-06) * norm_gain
    ).astype(BF16)
    routing = routing_rows(normed, router_weight, placement, expert_ids)
    own = [jnp.concatenate([normed, pack(routing, width)], 0)]
    for _ in range(1, steps):
        own.append(shift(own[-1], dims, "z", 1))

    last = own[:1]
    blocks, chosen, came, results, parts = {}, {}, {}, {}, {}
    firsts = [[o[0] for o in order] for order in orders]
    seconds = [[o[1] for o in order] for order in orders]
    for step in range(steps):
        chosen[step] = targets(dims, seconds[step])
        blocks[step] = [own[step]] + [
            shift(own[step], dims, firsts[step], d) for d in range(1, dims[firsts[step][0]])
        ]

    def send(step):
        nonlocal last
        sent = send_rows(blocks[step], chosen[step], shape, last)
        last = sent[:1]
        came[step] = [shift(r, dims, seconds[step], d + 1) for d, r in enumerate(sent)]

    def run(step):
        nonlocal last
        results[step] = feed_forward(
            blocks[step], came[step], expert_slices, chosen[step], shape, last
        )
        last = results[step][:1]

    def give(step):
        own_rows, *rest = results[step]
        results[step] = [own_rows] + [
            shift(r, dims, seconds[step], -d - 1) for d, r in enumerate(rest)
        ]

    def join(step, extra=()):
        nonlocal last
        out = combine(blocks[step], results[step], chosen[step], extra, shape, last)
        last = out[:1]
        parts[step] = out[:1] + [
            shift(r, dims, firsts[step], -d - 1) for d, r in enumerate(out[1:])
        ]

    def spread():
        nonlocal last, shared
        peers = [shift(b, dims, "c", d) for d in range(1, cores) for b in blocks[0]]
        shared = feed_forward(
            blocks[0], peers, [[shared_gate.T, shared_up.T, shared_down]], None, shape, last
        )
        last = shared[:1]
        shared = shared[:1] + [shift(r, dims, "c", -d - 1) for d, r in enumerate(shared[1:])]

    shared = []
    later = list(range(1, steps))
    for step in [0] + later[:1]:
        send(step)
    loaded = load([w for weights in expert_slices for w in weights], last)
    expert_slices = [loaded[i : i + 3] for i in range(0, len(loaded), 3)]
    last = loaded[-1:]
    spread()
    for step in later[1:2]:
        send(step)
    for step in later[:1]:
        run(step)
        give(step)
    for step in later[2:]:
        send(step)
    for step in later[1:2]:
        run(step)
        give(step)
    for step in later[:1]:
        join(step)
    for step in later[2:]:
        run(step)
        give(step)
    for step in later[1:2]:
        join(step)
    run(0)
    give(0)
    for step in later[2:]:
        join(step)
    join(0, shared)

    passed = []
    for step in later + [0]:
        total = parts[step][0]
        for part in parts[step][1:] + passed:
            total = total + part.astype(F32)
        total = total.astype(BF16)
        if step:
            passed = [shift(total, dims, "z", 1)]
    return total


def solution(mesh):
    in_specs = (
        P(AXES, None),
        P(),
        P(),
        P(),
        P(AXES, None),
        P(None, AXES),
        P(None, AXES),
        P(AXES, None),
        P(None, "local"),
        P(None, "local"),
        P("local", None),
    )
    out_specs = P(AXES, None)

    return jax.shard_map(body, mesh=mesh, in_specs=in_specs, out_specs=out_specs, check_vma=False)
```
